32 devices in a mesh: dp: 16 (over z, x, core), tensor: 2 (over y).
Axes of the slice: x: 2, y: 2, z: 4, core: 2. Of those that a mesh axis runs over, the one named last changes fastest.
Arguments:
- hidden_in: bfloat16 [6144, 4096], P('dp'), may hold values from -6 to 6
- upstream: bfloat16 [6144, 4096], P('dp'), may hold values from -6 to 6
- merged_input_weight: bfloat16 [4096, 6144], P('dp', 'tensor'), may hold values from -0.09375 to 0.09375
- output_matrix: bfloat16 [4096, 4096], P('dp', 'tensor'), may hold values from -0.09375 to 0.09375
- norm_gain: float32 [4096], replicated, may hold values from 0.5 to 1.5
- query_gain: float32 [128], replicated, may hold values from 0.5 to 1.5
- key_gain: float32 [128], replicated, may hold values from 0.5 to 1.5
Outputs:
- hidden_grad: bfloat16 [6144, 4096], P('dp')
- input_grad: float32 [4096, 6144], P('dp', 'tensor')
- output_grad: float32 [4096, 4096], P('dp', 'tensor')
- gain_grad: float32 [4096], replicated
- query_grad: float32 [128], replicated
- key_grad: float32 [128], replicated
The draws below stay inside these ranges and needn't reach their ends.
All inputs are finite; a program needn't handle non-finite values.
Results may differ from the reference program's by a relative error of at most 0.015.
Values may be sent and summed in bfloat16 or wider, within the bound.
A program may use at most 128 MiB of HBM per device.

```python
import math
from functools import partial
import jax
import jax.numpy as jnp
from jax import lax

MODEL_WIDTH = 4096
QUERY_HEADS = 32
KEY_VALUE_HEADS = 8
HEAD_SIZE = 128
SEQUENCE_LENGTH = 384
TOKENS = 6144
N_DP = 16
N_TENSOR = 2


def spiked(values, stream_key, source, target, shards_of, factor):
    def block_of(position):
        return (jnp.arange(values.shape[position]) // (values.shape[position] // shards_of)).reshape((-1,) + (1,) * (values.ndim - 1 - position))

    one_side = jax.random.permutation(stream_key, shards_of)[block_of(target)]
    second = (block_of(target) + shards_of // 2) % shards_of
    return jnp.where((block_of(source) == one_side) | (block_of(source) == second), factor * values, values)


def steps_of(key, dims, shards, least, largest):
    gain = 1.0
    for axis_at, shards_of in shards:
        steps = jax.random.uniform(jax.random.fold_in(jax.random.fold_in(key, 6), axis_at), (shards_of,), jnp.float32, least / len(shards), largest / len(shards))
        gain = gain * jnp.repeat(jnp.exp(steps), dims[axis_at] // shards_of).reshape((-1,) + (1,) * (len(dims) - 1 - axis_at))
    return gain


def gaussian(own_key, dims, spread, bound, shards=(), kind=jnp.bfloat16):
    array = jax.random.normal(own_key, dims, jnp.float32) * spread
    if len(shards) > 0:
        array = steps_of(own_key, dims, shards, -0.22, 0.18) * array
    return jnp.clip(array, min=-bound, max=bound).astype(kind)


def noise_with(stream_key, dims, scale, bound, split, heavy, held_as=jnp.bfloat16):
    drawn = scale * jax.random.normal(stream_key, dims, jnp.float32)
    if split:
        drawn = drawn * steps_of(stream_key, dims, split, -0.22, 0.18)
    return jnp.clip(spiked(drawn, jax.random.fold_in(stream_key, 3), *heavy), -bound, bound).astype(held_as)


def setup_inputs(seed: int = 0) -> dict:
    arg_keys = jax.random.split(jax.random.key(seed), 8)
    hidden_in = noise_with(arg_keys[0], (TOKENS, MODEL_WIDTH), 1.0, 6.0, ((0, 16),), (0, 1, 16, 2.0))
    upstream = noise_with(arg_keys[1], (TOKENS, MODEL_WIDTH), 1.0, 6.0, ((0, 16),), (0, 1, 16, 2.0))
    merged_input_weight = gaussian(arg_keys[2], (MODEL_WIDTH, (QUERY_HEADS + 2 * KEY_VALUE_HEADS) * HEAD_SIZE), MODEL_WIDTH ** -0.5, 0.09375, ((0, 16), (1, 2)))
    output_matrix = gaussian(arg_keys[3], (MODEL_WIDTH, QUERY_HEADS * HEAD_SIZE), (QUERY_HEADS * HEAD_SIZE) ** -0.5, 0.09375, ((0, 16), (1, 2)))
    norm_gain = jnp.clip(1.0 + 0.1 * jax.random.normal(arg_keys[4], (MODEL_WIDTH,), jnp.float32), 0.5, 1.5)
    query_gain = jnp.clip(1.0 + 0.1 * jax.random.normal(arg_keys[5], (HEAD_SIZE,), jnp.float32), 0.5, 1.5)
    key_gain = jnp.clip(1.0 + 0.1 * jax.random.normal(arg_keys[6], (HEAD_SIZE,), jnp.float32), 0.5, 1.5)
    return {"hidden_in": hidden_in, "upstream": upstream, "merged_input_weight": merged_input_weight, "output_matrix": output_matrix, "norm_gain": norm_gain, "query_gain": query_gain, "key_gain": key_gain}


EPSILON = 1e-06
ROPE_BASE = 1000000.0

def lowered_precision(value_rows):
    return lax.optimization_barrier(value_rows.astype(jnp.bfloat16))

def norm_rows(states, scaling):
    widened = states.astype(jnp.float32)
    inverse = lax.rsqrt(lax.optimization_barrier(jnp.mean(widened * widened, axis=-1, keepdims=True)) + EPSILON)
    return widened * inverse * scaling

def rope_tables(length, columns):
    half_width = columns // 2
    exponent = jnp.arange(half_width, dtype=jnp.float32) * (2.0 / columns)
    frequency = jnp.exp(-exponent * math.log(ROPE_BASE))
    places = jnp.arange(length, dtype=jnp.float32)
    angles = places[:, None] * frequency[None, :]
    return (jnp.cos(angles), jnp.sin(angles))

def head_post(projected_rows, scaling, cosine, sine):
    inverse = lax.rsqrt(lax.optimization_barrier(jnp.mean(projected_rows * projected_rows, axis=-1, keepdims=True)) + EPSILON)
    normed = projected_rows * inverse * scaling
    half_width = projected_rows.shape[-1] // 2
    layout = (projected_rows.shape[0],) + (1,) * (projected_rows.ndim - 2) + (half_width,)
    cosine_part = cosine.reshape(layout)
    sine_part = sine.reshape(layout)
    leading = normed[..., :half_width]
    trailing = normed[..., half_width:]
    return jnp.concatenate([leading * cosine_part - trailing * sine_part, trailing * cosine_part + leading * sine_part], axis=-1)

def widen(value_rows):
    return value_rows.astype(jnp.float32)

def reference(hidden_in, upstream, merged_input_weight, output_matrix, norm_gain, query_gain, key_gain):
    shard_ranks = N_TENSOR
    query_heads = QUERY_HEADS // shard_ranks
    key_head_rows = KEY_VALUE_HEADS // shard_ranks
    group_width = QUERY_HEADS // KEY_VALUE_HEADS
    attention_block = (QUERY_HEADS + 2 * KEY_VALUE_HEADS) * HEAD_SIZE // shard_ranks
    query_columns = query_heads * HEAD_SIZE
    key_columns = key_head_rows * HEAD_SIZE
    grad_scale = 1.0 / math.sqrt(TOKENS)
    score_scale = 1.0 / math.sqrt(HEAD_SIZE)
    cosine, sine = rope_tables(SEQUENCE_LENGTH, HEAD_SIZE)
    post = partial(head_post, cosine=cosine, sine=sine)
    weight_blocks = merged_input_weight.astype(jnp.float32).reshape(MODEL_WIDTH, shard_ranks, attention_block)
    causal = lax.broadcasted_iota(jnp.int32, (SEQUENCE_LENGTH, SEQUENCE_LENGTH), 0) >= lax.broadcasted_iota(jnp.int32, (SEQUENCE_LENGTH, SEQUENCE_LENGTH), 1)

    def one_sequence(carry, inputs):
        input_acc, output_acc, gain_acc, query_acc, key_acc = carry
        hidden, incoming_gradient = inputs
        local_norm, norm_back = jax.vjp(norm_rows, hidden.astype(jnp.float32), norm_gain)
        normed = lowered_precision(local_norm)
        projected_rows = jnp.dot(normed, merged_input_weight, preferred_element_type=jnp.float32).reshape(SEQUENCE_LENGTH, shard_ranks, attention_block)
        unnormed_query = projected_rows[:, :, :query_columns].reshape(SEQUENCE_LENGTH, KEY_VALUE_HEADS, group_width, HEAD_SIZE)
        unnormed_key = projected_rows[:, :, query_columns:query_columns + key_columns].reshape(SEQUENCE_LENGTH, KEY_VALUE_HEADS, HEAD_SIZE)
        value_rows = lowered_precision(projected_rows[:, :, query_columns + key_columns:].reshape(SEQUENCE_LENGTH, KEY_VALUE_HEADS, HEAD_SIZE))
        queries_full, query_back = jax.vjp(post, unnormed_query, query_gain)
        keys_full, key_back = jax.vjp(post, unnormed_key, key_gain)
        queries = lowered_precision(queries_full)
        keys = lowered_precision(keys_full)
        scores = jnp.einsum('tkgh,skh->kgts', widen(queries), widen(keys)) * score_scale
        raised = jnp.where(causal, jnp.exp(scores), 0.0)
        softmax = raised / lax.optimization_barrier(jnp.sum(raised, axis=-1, keepdims=True))
        softmax_low = lowered_precision(softmax)
        context = jnp.einsum('kgts,skh->tkgh', widen(softmax_low), widen(value_rows))
        context_low = lowered_precision(context).reshape(SEQUENCE_LENGTH, QUERY_HEADS * HEAD_SIZE)
        context_gradient = lowered_precision(jnp.dot(incoming_gradient, output_matrix, preferred_element_type=jnp.float32)).reshape(SEQUENCE_LENGTH, KEY_VALUE_HEADS, group_width, HEAD_SIZE)
        grad_probs = jnp.einsum('tkgh,skh->kgts', widen(context_gradient), widen(value_rows))
        centre = lax.optimization_barrier(jnp.sum(softmax * grad_probs, axis=-1, keepdims=True))
        grad_scores = lowered_precision(softmax * (grad_probs - centre) * score_scale)
        grad_values = jnp.einsum('kgts,tkgh->skh', widen(softmax_low), widen(context_gradient))
        grad_queries = jnp.einsum('kgts,skh->tkgh', widen(grad_scores), widen(keys))
        grad_keys = jnp.einsum('kgts,tkgh->skh', widen(grad_scores), widen(queries))
        grad_raw_query, query_part = query_back(grad_queries)
        grad_raw_key, key_part = key_back(grad_keys)
        grad_projected = lowered_precision(jnp.concatenate([grad_raw_query.reshape(SEQUENCE_LENGTH, shard_ranks, query_columns), grad_raw_key.reshape(SEQUENCE_LENGTH, shard_ranks, key_columns), grad_values.reshape(SEQUENCE_LENGTH, shard_ranks, key_columns)], axis=2).reshape(SEQUENCE_LENGTH, shard_ranks * attention_block))
        input_term = lowered_precision(jnp.dot(normed.T, grad_projected, preferred_element_type=jnp.float32) * grad_scale)
        output_term = lowered_precision(jnp.dot(incoming_gradient.T, context_low, preferred_element_type=jnp.float32) * grad_scale)
        rank_terms = jnp.einsum('trc,drc->rtd', widen(grad_projected).reshape(SEQUENCE_LENGTH, shard_ranks, attention_block), weight_blocks)
        grad_normed = lax.optimization_barrier(jnp.sum(widen(lowered_precision(rank_terms)), axis=0))
        grad_hidden, gain_part = norm_back(grad_normed)
        hidden_grad = (incoming_gradient.astype(jnp.float32) + grad_hidden).astype(jnp.bfloat16)
        carry = (input_acc + widen(input_term), output_acc + widen(output_term), gain_acc + gain_part, query_acc + query_part, key_acc + key_part)
        return (carry, hidden_grad)
    start_offset = (jnp.zeros((MODEL_WIDTH, (QUERY_HEADS + 2 * KEY_VALUE_HEADS) * HEAD_SIZE), jnp.float32), jnp.zeros((MODEL_WIDTH, QUERY_HEADS * HEAD_SIZE), jnp.float32), jnp.zeros((MODEL_WIDTH,), jnp.float32), jnp.zeros((HEAD_SIZE,), jnp.float32), jnp.zeros((HEAD_SIZE,), jnp.float32))
    sequences = (hidden_in.reshape(N_DP, SEQUENCE_LENGTH, MODEL_WIDTH), upstream.reshape(N_DP, SEQUENCE_LENGTH, MODEL_WIDTH))
    totals, hidden_parts = lax.scan(one_sequence, start_offset, sequences)
    input_grad, output_grad, gain_sum, query_sum, key_sum = totals
    return (hidden_parts.reshape(TOKENS, MODEL_WIDTH), input_grad, output_grad, gain_sum * grad_scale, query_sum * grad_scale, key_sum * grad_scale)
```

```python
from functools import partial
import math

import jax
import jax.numpy as jnp
from jax import lax
from jax.experimental import pallas as pl
from jax.experimental.pallas import tpu as pltpu
from jax.sharding import PartitionSpec as P

QUERY_HEADS = 32
KEY_VALUE_HEADS = 8
HEAD_SIZE = 128


EPSILON = 1e-06
ROPE_BASE = 1000000.0
F32 = jnp.float32
BF16 = jnp.bfloat16


def norm_rows(states, scaling):
    inverse = lax.rsqrt(jnp.mean(states * states, axis=-1, keepdims=True) + EPSILON)
    return states * inverse * scaling


def rope_tables(length, columns):
    half_width = columns // 2
    exponent = jnp.arange(half_width, dtype=jnp.float32) * (2.0 / columns)
    frequency = jnp.exp(-exponent * math.log(ROPE_BASE))
    places = jnp.arange(length, dtype=jnp.float32)
    angles = places[:, None] * frequency[None, :]
    return (jnp.cos(angles), jnp.sin(angles))


def head_post(projected_rows, scaling, cosine, sine):
    inverse = lax.rsqrt(jnp.mean(projected_rows * projected_rows, axis=-1, keepdims=True) + EPSILON)
    normed = projected_rows * inverse * scaling
    half_width = projected_rows.shape[-1] // 2
    layout = (projected_rows.shape[0],) + (1,) * (projected_rows.ndim - 2) + (half_width,)
    cosine_part = cosine.reshape(layout)
    sine_part = sine.reshape(layout)
    leading = normed[..., :half_width]
    trailing = normed[..., half_width:]
    return jnp.concatenate(
        [
            leading * cosine_part - trailing * sine_part,
            trailing * cosine_part + leading * sine_part,
        ],
        axis=-1,
    )


def attend_forward(queries, keys, value_rows, score_scale):
    length = queries.shape[0]
    scores = (
        jnp.einsum("tkgh,skh->kgts", queries, keys, preferred_element_type=jnp.float32)
        * score_scale
    )
    causal = lax.broadcasted_iota(jnp.int32, (length, length), 0) >= lax.broadcasted_iota(
        jnp.int32, (length, length), 1
    )
    raised = jnp.where(causal, jnp.exp(scores), 0.0)
    softmax = raised / jnp.sum(raised, axis=-1, keepdims=True)
    softmax_low = softmax.astype(jnp.bfloat16)
    context = jnp.einsum(
        "kgts,skh->tkgh", softmax_low, value_rows, preferred_element_type=jnp.float32
    )
    return (softmax, softmax_low, context)


def attend_backward(queries, keys, value_rows, softmax, softmax_low, context_gradient, score_scale):
    grad_probs = jnp.einsum(
        "tkgh,skh->kgts", context_gradient, value_rows, preferred_element_type=jnp.float32
    )
    centre = jnp.sum(softmax * grad_probs, axis=-1, keepdims=True)
    grad_scores = (softmax * (grad_probs - centre) * score_scale).astype(jnp.bfloat16)
    grad_values = jnp.einsum(
        "kgts,tkgh->skh", softmax_low, context_gradient, preferred_element_type=jnp.float32
    )
    grad_queries = jnp.einsum(
        "kgts,skh->tkgh", grad_scores, keys, preferred_element_type=jnp.float32
    )
    grad_keys = jnp.einsum(
        "kgts,tkgh->skh", grad_scores, queries, preferred_element_type=jnp.float32
    )
    return (grad_queries, grad_keys, grad_values)


def device_bits(count):
    bits = []
    bit = 1
    while bit < count:
        bits.append(bit)
        bit *= 2
    return bits


def swap(values, bit):
    count = lax.axis_size("dp")
    return lax.ppermute(values, "dp", [(i, i ^ bit) for i in range(count)])


def swap_tensor(values):
    return lax.ppermute(values, "tensor", [(0, 1), (1, 0)])


def bit_of(index, bit):
    return (index // bit) % 2


def ordered(flag, own, other, axis):
    return jnp.where(
        flag == 0,
        jnp.concatenate([own, other], axis),
        jnp.concatenate([other, own], axis),
    )


def half_rows(values, flag):
    half = values.shape[0] // 2
    return lax.dynamic_slice_in_dim(values, flag * half, half, 0)


def sum_all(values, axis):
    count = lax.axis_size(axis)
    if count & (count - 1):
        return lax.psum(values, axis)
    step = 1
    while step < count:
        values = values + lax.ppermute(values, axis, [(i, i ^ step) for i in range(count)])
        step *= 2
    return values


def block_places(bits_inner, bits_outer, device):
    places = [(0, 0)]
    for bit in reversed(bits_inner):
        places = places + [(fixed | bit, relative) for fixed, relative in places]
    for bit in bits_outer:
        places = places + [(fixed, relative | bit) for fixed, relative in places]
    mask = sum(bits_outer)
    return [fixed + jnp.bitwise_xor(relative, jnp.bitwise_and(device, mask)) for fixed, relative in places]


def permute_columns(values, places):
    width = values.shape[1] // len(places)
    return jnp.concatenate(
        [lax.dynamic_slice_in_dim(values, place * width, width, 1) for place in places], axis=1
    )


def restore_columns(values, places):
    width = values.shape[1] // len(places)
    result = jnp.zeros_like(values)
    for at, place in enumerate(places):
        result = lax.dynamic_update_slice_in_dim(
            result, values[:, at * width : (at + 1) * width], place * width, 1
        )
    return result


def split_heads(shard, head_bits, device):
    held = shard
    for bit in reversed(head_bits):
        flag = bit_of(device, bit)
        count = held.shape[0] // 2
        kept = lax.dynamic_slice_in_dim(held, flag * count, count, 0)
        sent = lax.dynamic_slice_in_dim(held, (1 - flag) * count, count, 0)
        got = swap(sent, bit)
        held = ordered(flag, kept, got, 1)
    return held[0]


def gather_rows(held, outer_bits):
    for bit in outer_bits:
        held = jnp.concatenate([held, swap(held, bit)], axis=0)
    return held


def sum_rows(left, right, outer_bits):
    def term(first, last):
        return lax.dot_general(
            left[:, first:last], right, (((0,), (0,)), ((), ())), preferred_element_type=F32
        )

    rows = left.shape[1]
    half = rows // 2
    sent = term(half, rows).astype(BF16)
    got = swap(sent, outer_bits[-1])
    held = term(0, half) + got.astype(F32)
    for bit in reversed(outer_bits[:-1]):
        half = held.shape[0] // 2
        got = swap(held[half:].astype(BF16), bit)
        held = held[:half] + got.astype(F32)
    return held


def join_heads(held, head_bits, device):
    parts = 2 ** len(head_bits)
    if parts == 1:
        return held[None]
    held = held.astype(BF16).reshape(1, held.shape[0], held.shape[1])
    for bit in head_bits:
        flag = bit_of(device, bit)
        half = held.shape[1] // 2
        kept = lax.dynamic_slice_in_dim(held, flag * half, half, 1)
        sent = lax.dynamic_slice_in_dim(held, (1 - flag) * half, half, 1)
        got = swap(sent, bit)
        held = ordered(flag, kept[None], got[None], 0)
        held = held.reshape(-1, half, held.shape[-1])
    return held


def local(hidden_in, upstream, merged_input_weight, output_matrix, norm_gain, query_gain, key_gain):
    shard_ranks = lax.axis_size("tensor")
    groups = lax.axis_size("dp")
    device = lax.axis_index("dp")
    query_heads = QUERY_HEADS // shard_ranks
    key_heads = KEY_VALUE_HEADS // shard_ranks
    group_width = QUERY_HEADS // KEY_VALUE_HEADS
    score_scale = 1.0 / math.sqrt(HEAD_SIZE)
    length, model = hidden_in.shape
    grad_scale = 1.0 / math.sqrt(groups * length)
    bits = device_bits(groups)
    head_bits = []
    for bit in (1, 4):
        if bit in bits and key_heads % (2 ** (len(head_bits) + 1)) == 0:
            head_bits.append(bit)
    outer_bits = [bit for bit in bits if bit > 2 and bit not in head_bits]
    outer_bits += [bit for bit in bits if bit <= 2 and bit not in head_bits]
    parts = 2 ** len(head_bits)
    places = block_places(head_bits, outer_bits, device)
    part_queries = query_heads // parts
    part_keys = key_heads // parts
    query_columns = part_queries * HEAD_SIZE
    key_columns = part_keys * HEAD_SIZE
    plane = lax.axis_index("tensor")

    rows = merged_input_weight.shape[0]
    q_all, k_all = query_heads * HEAD_SIZE, key_heads * HEAD_SIZE
    weight_parts = jnp.concatenate(
        [
            merged_input_weight[:, :q_all].reshape(rows, parts, query_columns),
            merged_input_weight[:, q_all : q_all + k_all].reshape(rows, parts, key_columns),
            merged_input_weight[:, q_all + k_all :].reshape(rows, parts, key_columns),
        ],
        axis=2,
    ).transpose(1, 0, 2)
    weight_held = split_heads(weight_parts, head_bits, device)

    def share_tokens(own):
        held = [own]
        for bit in reversed(head_bits):
            if bit == 1 or shard_ranks != 2:
                held = held + [swap(one, bit) for one in held]
            else:
                fresh = []
                for one in held:
                    got = swap(half_rows(one, plane), bit)
                    fresh.append(ordered(plane, got, swap_tensor(got), 0))
                held = held + fresh
        return jnp.concatenate(held, axis=0)

    local_norm, norm_back = jax.vjp(norm_rows, hidden_in.astype(F32), norm_gain)
    normed = permute_columns(local_norm.astype(BF16), places)
    normed_all = share_tokens(normed)

    chunk = 2 * HEAD_SIZE
    weight_chunks = []
    for at in range(0, weight_held.shape[1], chunk):
        weight_chunks.append(gather_rows(weight_held[:, at : at + chunk], outer_bits))
    matrix_parts = output_matrix.reshape(rows, parts, query_columns).transpose(1, 0, 2)
    matrix_held = split_heads(matrix_parts, head_bits, device)
    upstream_all = share_tokens(permute_columns(upstream, places))
    matrix_chunks = []
    for at in range(0, matrix_held.shape[1], chunk):
        matrix_chunks.append(gather_rows(matrix_held[:, at : at + chunk], outer_bits))

    projected = jnp.concatenate(
        [jnp.dot(normed_all, one, preferred_element_type=F32) for one in weight_chunks], axis=1
    )
    sequences = parts
    unnormed_query = projected[:, :query_columns].reshape(
        sequences, length, part_keys, group_width, HEAD_SIZE
    )
    unnormed_key = projected[:, query_columns : query_columns + key_columns].reshape(
        sequences, length, part_keys, HEAD_SIZE
    )
    value_rows = (
        projected[:, query_columns + key_columns :]
        .astype(BF16)
        .reshape(sequences, length, part_keys, HEAD_SIZE)
    )
    cosine, sine = rope_tables(length, HEAD_SIZE)

    def post(raw, gain):
        return jax.vmap(lambda one: head_post(one, gain, cosine, sine))(raw)

    queries_full, query_back = jax.vjp(post, unnormed_query, query_gain)
    keys_full, key_back = jax.vjp(post, unnormed_key, key_gain)
    queries = queries_full.astype(BF16)
    keys = keys_full.astype(BF16)
    softmax, softmax_low, context = jax.vmap(partial(attend_forward, score_scale=score_scale))(
        queries, keys, value_rows
    )
    context_low = context.astype(BF16).reshape(sequences * length, query_columns)
    output_sums = jnp.concatenate(
        [
            sum_rows(upstream_all, context_low[:, at : at + chunk], outer_bits)
            for at in range(0, query_columns, chunk)
        ],
        axis=1,
    )
    output_parts = join_heads(output_sums, head_bits, device).astype(F32)
    output_grad = output_parts.transpose(1, 0, 2).reshape(rows, q_all) * grad_scale

    context_gradient = jnp.concatenate(
        [
            jnp.dot(upstream_all, one, preferred_element_type=F32).astype(BF16)
            for one in matrix_chunks
        ],
        axis=1,
    ).reshape(sequences, length, part_keys, group_width, HEAD_SIZE)
    grad_queries, grad_keys, grad_values = jax.vmap(
        partial(attend_backward, score_scale=score_scale)
    )(queries, keys, value_rows, softmax, softmax_low, context_gradient)
    grad_raw_query, query_part = query_back(grad_queries)
    grad_raw_key, key_part = key_back(grad_keys)
    grad_projected = jnp.concatenate(
        [
            grad_raw_query.reshape(sequences * length, query_columns),
            grad_raw_key.reshape(sequences * length, key_columns),
            grad_values.reshape(sequences * length, key_columns),
        ],
        axis=1,
    ).astype(BF16)

    weight_full = jnp.concatenate(weight_chunks, axis=1)
    share = lax.dot_general(
        grad_projected, weight_full, (((1,), (1,)), ((), ())), preferred_element_type=F32
    ).astype(BF16)
    input_sums = jnp.concatenate(
        [
            sum_rows(normed_all, grad_projected[:, at : at + chunk], outer_bits)
            for at in range(0, grad_projected.shape[1], chunk)
        ],
        axis=1,
    )
    input_parts = join_heads(input_sums, head_bits, device).astype(F32) * grad_scale
    input_grad = jnp.concatenate(
        [
            input_parts[:, :, :query_columns].transpose(1, 0, 2).reshape(rows, q_all),
            input_parts[:, :, query_columns : query_columns + key_columns]
            .transpose(1, 0, 2)
            .reshape(rows, k_all),
            input_parts[:, :, query_columns + key_columns :].transpose(1, 0, 2).reshape(rows, k_all),
        ],
        axis=1,
    )

    held = [share[i * length : (i + 1) * length] for i in range(parts)]
    for bit in head_bits:
        half = len(held) // 2
        if bit == 1 or shard_ranks != 2:
            got = [swap(one.astype(BF16), bit) for one in held[half:]]
            held = [one.astype(F32) + other.astype(F32) for one, other in zip(held[:half], got)]
        else:
            fresh = []
            for one, away in zip(held[:half], held[half:]):
                mine = half_rows(away, plane).astype(F32)
                got = swap_tensor(half_rows(away, 1 - plane).astype(BF16))
                back = swap((mine + got.astype(F32)).astype(BF16), bit)
                zero = jnp.zeros_like(back)
                spread = jnp.where(
                    plane == 0,
                    jnp.concatenate([back, zero], 0),
                    jnp.concatenate([zero, back], 0),
                )
                fresh.append(one.astype(F32) + spread.astype(F32))
            held = fresh
    partial_normed = held[0].astype(BF16)
    grad_normed = partial_normed.astype(F32)
    for shift in range(1, shard_ranks):
        grad_normed = grad_normed + lax.ppermute(
            partial_normed, "tensor", [(i, (i + shift) % shard_ranks) for i in range(shard_ranks)]
        ).astype(F32)
    grad_normed = restore_columns(grad_normed, places)
    grad_hidden, gain_part = norm_back(grad_normed)
    hidden_grad = (upstream.astype(F32) + grad_hidden).astype(BF16)
    gains = jnp.concatenate([gain_part * (1.0 / shard_ranks), query_part, key_part])
    gains = sum_all(sum_all(gains, "tensor"), "dp")
    gain_sum, query_sum, key_sum = jnp.split(gains, [model, model + HEAD_SIZE])
    return (
        hidden_grad,
        input_grad,
        output_grad,
        gain_sum * grad_scale,
        query_sum * grad_scale,
        key_sum * grad_scale,
    )


def solution(mesh):
    in_specs = (P("dp", None), P("dp", None), P("dp", "tensor"), P("dp", "tensor"), P(), P(), P())
    out_specs = (P("dp", None), P("dp", "tensor"), P("dp", "tensor"), P(), P(), P())
    return jax.shard_map(local, mesh=mesh, in_specs=in_specs, out_specs=out_specs, check_vma=False)
```

```python
from functools import partial
import math

import jax
import jax.numpy as jnp
from jax import lax
from jax.experimental import pallas as pl
from jax.experimental.pallas import tpu as pltpu
from jax.sharding import PartitionSpec as P

QUERY_HEADS = 32
KEY_VALUE_HEADS = 8
HEAD_SIZE = 128


EPSILON = 1e-06
ROPE_BASE = 1000000.0
F32 = jnp.float32
BF16 = jnp.bfloat16
ROW_BLOCK = 128
MESH = pl.DeviceIdType.MESH


def rope_tables(length, columns):
    half_width = columns // 2
    exponent = jnp.arange(half_width, dtype=jnp.float32) * (2.0 / columns)
    frequency = jnp.exp(-exponent * math.log(ROPE_BASE))
    places = jnp.arange(length, dtype=jnp.float32)
    angles = places[:, None] * frequency[None, :]
    cosine, sine = jnp.cos(angles), jnp.sin(angles)
    return (
        jnp.concatenate([cosine, cosine], axis=1),
        jnp.concatenate([-sine, sine], axis=1),
    )


def call_params(vmem_mib):
    return pltpu.CompilerParams(
        dimension_semantics=("arbitrary",), vmem_limit_bytes=vmem_mib * 1024 * 1024
    )


def leave_kernel(places_ref, hidden_ref, upstream_ref, gain_ref, *rest):
    *shares, grad_ref, gain_grad_ref, natural = rest
    count = places_ref.shape[0]
    width = hidden_ref.shape[1] // count
    for at in range(count):
        target = pl.ds(pl.multiple_of(places_ref[at] * width, width), width)
        source = slice(at * width, (at + 1) * width)
        total = shares[0][:, source].astype(F32)
        for other in shares[1:]:
            total = total + other[:, source].astype(F32)
        natural[:, target] = total
    states = hidden_ref[...].astype(F32)
    inverse = lax.rsqrt(jnp.mean(states * states, axis=-1, keepdims=True) + EPSILON)
    unit = states * inverse
    part = jnp.sum(natural[...] * unit, axis=0, keepdims=True)

    @pl.when(pl.program_id(0) == 0)
    def _():
        gain_grad_ref[...] = part

    @pl.when(pl.program_id(0) != 0)
    def _():
        gain_grad_ref[...] += part

    scaled = natural[...] * gain_ref[...]
    mean = jnp.mean(scaled * unit, axis=-1, keepdims=True)
    grad = inverse * (scaled - unit * mean)
    grad_ref[...] = (upstream_ref[...].astype(F32) + grad).astype(BF16)


def leave(places, hidden_in, upstream, norm_gain, shares):
    length, model = hidden_in.shape
    block = min(length, ROW_BLOCK)
    whole = pl.BlockSpec((block, model), lambda i, places: (i, 0))
    line = pl.BlockSpec((1, model), lambda i, places: (0, 0))
    hidden_grad, gain_part = pl.pallas_call(
        leave_kernel,
        grid_spec=pltpu.PrefetchScalarGridSpec(
            num_scalar_prefetch=1,
            grid=(length // block,),
            in_specs=[whole, whole, line] + [whole] * len(shares),
            out_specs=[whole, line],
            scratch_shapes=[pltpu.VMEM((block, model), F32)],
        ),
        out_shape=[
            jax.ShapeDtypeStruct((length, model), BF16),
            jax.ShapeDtypeStruct((1, model), F32),
        ],
        compiler_params=call_params(40),
        cost_estimate=pl.CostEstimate(
            flops=12 * length * model,
            bytes_accessed=(6 + 2 * len(shares)) * length * model,
            transcendentals=length,
        ),
        name="leave",
    )(places, hidden_in, upstream, norm_gain.reshape(1, model), *shares)
    return hidden_grad, gain_part[0]


def turn(values):
    return pltpu.roll(values, HEAD_SIZE // 2, 1)


def head_states(raw, gain, cosine, sine):
    inverse = lax.rsqrt(jnp.mean(raw * raw, axis=-1, keepdims=True) + EPSILON)
    normed = raw * inverse * gain
    return (normed * cosine + turn(normed) * sine).astype(BF16)


def head_back(grad, raw, gain, cosine, sine):
    inverse = lax.rsqrt(jnp.mean(raw * raw, axis=-1, keepdims=True) + EPSILON)
    unit = raw * inverse
    grad_normed = grad * cosine + turn(grad * sine)
    part = jnp.sum(grad_normed * unit, axis=0, keepdims=True)
    scaled = grad_normed * gain
    mean = jnp.mean(scaled * unit, axis=-1, keepdims=True)
    return inverse * (scaled - unit * mean), part


def columns_of(index):
    return slice(index * HEAD_SIZE, (index + 1) * HEAD_SIZE)


def matmul(left, right, contract):
    return lax.dot_general(left, right, ((contract[:1], contract[1:]), ((), ())), preferred_element_type=F32)


def block_probs(queries, keys, tile, width, scale):
    scores = matmul(queries, keys, (1, 1)) * scale
    height = scores.shape[0]
    at_row = lax.rem(lax.broadcasted_iota(jnp.int32, (height, width), 0), tile) + (width - tile)
    causal = at_row >= lax.broadcasted_iota(jnp.int32, (height, width), 1)
    raised = jnp.where(causal, jnp.exp(scores), 0.0)
    return raised / jnp.sum(raised, axis=-1, keepdims=True)


def forward_kernel(heads, group, tile, raw_ref, gains_ref, cosine_ref, sine_ref, context_ref):
    length = raw_ref.shape[0]
    query_total = heads * group
    scale = 1.0 / math.sqrt(HEAD_SIZE)
    for head in range(heads):
        keys = head_states(
            raw_ref[:, columns_of(query_total + head)], gains_ref[1:2], cosine_ref[...], sine_ref[...]
        )
        values = raw_ref[:, columns_of(query_total + heads + head)].astype(BF16)
        for start in range(0, length, tile):
            rows = slice(start, start + tile)
            width = start + tile
            queries = jnp.concatenate(
                [
                    head_states(
                        raw_ref[rows, columns_of(head * group + one)],
                        gains_ref[0:1],
                        cosine_ref[rows],
                        sine_ref[rows],
                    )
                    for one in range(group)
                ],
                axis=0,
            )
            probs = block_probs(queries, keys[:width], tile, width, scale)
            context = matmul(probs.astype(BF16), values[:width], (1, 0)).astype(BF16)
            for one in range(group):
                context_ref[rows, columns_of(head * group + one)] = context[one * tile : (one + 1) * tile]


def backward_kernel(
    heads, group, tile, raw_ref, grad_ref, gains_ref, cosine_ref, sine_ref, out_ref, sums_ref
):
    length = raw_ref.shape[0]
    query_total = heads * group
    scale = 1.0 / math.sqrt(HEAD_SIZE)
    query_sum = jnp.zeros((1, HEAD_SIZE), F32)
    key_sum = jnp.zeros((1, HEAD_SIZE), F32)
    for head in range(heads):
        raw_keys = raw_ref[:, columns_of(query_total + head)]
        keys = head_states(raw_keys, gains_ref[1:2], cosine_ref[...], sine_ref[...])
        values = raw_ref[:, columns_of(query_total + heads + head)].astype(BF16)
        grad_keys = [jnp.zeros((tile, HEAD_SIZE), F32) for _ in range(length // tile)]
        grad_values = [jnp.zeros((tile, HEAD_SIZE), F32) for _ in range(length // tile)]
        for start in range(0, length, tile):
            rows = slice(start, start + tile)
            width = start + tile
            raw = jnp.concatenate(
                [raw_ref[rows, columns_of(head * group + one)] for one in range(group)], axis=0
            )
            cosine = jnp.concatenate([cosine_ref[rows]] * group, axis=0)
            sine = jnp.concatenate([sine_ref[rows]] * group, axis=0)
            queries = head_states(raw, gains_ref[0:1], cosine, sine)
            probs = block_probs(queries, keys[:width], tile, width, scale)
            probs_low = probs.astype(BF16)
            context_grad = jnp.concatenate(
                [grad_ref[rows, columns_of(head * group + one)] for one in range(group)], axis=0
            )
            grad_probs = matmul(context_grad, values[:width], (1, 1))
            centre = jnp.sum(probs * grad_probs, axis=-1, keepdims=True)
            grad_scores = (probs * (grad_probs - centre) * scale).astype(BF16)
            part_values = matmul(probs_low, context_grad, (0, 0))
            part_keys = matmul(grad_scores, queries, (0, 0))
            for at in range(width // tile):
                piece = slice(at * tile, (at + 1) * tile)
                grad_values[at] = grad_values[at] + part_values[piece]
                grad_keys[at] = grad_keys[at] + part_keys[piece]
            grad_queries = matmul(grad_scores, keys[:width], (1, 0))
            grad_raw, part = head_back(grad_queries, raw, gains_ref[0:1], cosine, sine)
            query_sum = query_sum + part
            grad_raw = grad_raw.astype(BF16)
            for one in range(group):
                out_ref[rows, columns_of(head * group + one)] = grad_raw[one * tile : (one + 1) * tile]
        grad_raw, part = head_back(
            jnp.concatenate(grad_keys, axis=0), raw_keys, gains_ref[1:2], cosine_ref[...], sine_ref[...]
        )
        key_sum = key_sum + part
        out_ref[:, columns_of(query_total + head)] = grad_raw.astype(BF16)
        out_ref[:, columns_of(query_total + heads + head)] = jnp.concatenate(
            grad_values, axis=0
        ).astype(BF16)
    sums = jnp.concatenate([query_sum, key_sum], axis=0)

    @pl.when(pl.program_id(0) == 0)
    def _():
        sums_ref[...] = sums

    @pl.when(pl.program_id(0) != 0)
    def _():
        sums_ref[...] += sums


def attention_specs(length, heads, group):
    return (
        pl.BlockSpec((length, (heads * group + 2 * heads) * HEAD_SIZE), lambda i: (i, 0)),
        pl.BlockSpec((length, heads * group * HEAD_SIZE), lambda i: (i, 0)),
        pl.BlockSpec((2, HEAD_SIZE), lambda i: (0, 0)),
        pl.BlockSpec((length, HEAD_SIZE), lambda i: (0, 0)),
    )


def attention_forward(raw, gains, cosine, sine, heads, group):
    length = cosine.shape[0]
    sequences = raw.shape[0] // length
    raw_spec, head_spec, gain_spec, table_spec = attention_specs(length, heads, group)
    pairs = sequences * heads * group * length * length
    return pl.pallas_call(
        partial(forward_kernel, heads, group, min(length, ROW_BLOCK)),
        grid=(sequences,),
        in_specs=[raw_spec, gain_spec, table_spec, table_spec],
        out_specs=head_spec,
        out_shape=jax.ShapeDtypeStruct((raw.shape[0], heads * group * HEAD_SIZE), BF16),
        compiler_params=call_params(40),
        cost_estimate=pl.CostEstimate(
            flops=8 * pairs * HEAD_SIZE, bytes_accessed=raw.size * 6, transcendentals=pairs
        ),
        name="attention_forward",
    )(raw, gains, cosine, sine)


def attention_backward(raw, context_grad, gains, cosine, sine, heads, group):
    length = cosine.shape[0]
    sequences = raw.shape[0] // length
    raw_spec, head_spec, gain_spec, table_spec = attention_specs(length, heads, group)
    pairs = sequences * heads * group * length * length
    return pl.pallas_call(
        partial(backward_kernel, heads, group, min(length, ROW_BLOCK)),
        grid=(sequences,),
        in_specs=[raw_spec, head_spec, gain_spec, table_spec, table_spec],
        out_specs=[raw_spec, gain_spec],
        out_shape=[
            jax.ShapeDtypeStruct(raw.shape, BF16),
            jax.ShapeDtypeStruct((2, HEAD_SIZE), F32),
        ],
        compiler_params=call_params(48),
        cost_estimate=pl.CostEstimate(
            flops=20 * pairs * HEAD_SIZE, bytes_accessed=raw.size * 8, transcendentals=pairs
        ),
        name="attention_backward",
    )(raw, context_grad, gains, cosine, sine)


def device_bits(count):
    bits = []
    bit = 1
    while bit < count:
        bits.append(bit)
        bit *= 2
    return bits


def swap(values, bit):
    count = lax.axis_size("dp")
    return lax.ppermute(values, "dp", [(i, i ^ bit) for i in range(count)])


def swap_tensor(values):
    return lax.ppermute(values, "tensor", [(0, 1), (1, 0)])


def bit_of(index, bit):
    return (index // bit) % 2


def ordered(flag, own, other, axis):
    return jnp.where(
        flag == 0,
        jnp.concatenate([own, other], axis),
        jnp.concatenate([other, own], axis),
    )


def half_rows(values, flag):
    half = values.shape[0] // 2
    return lax.dynamic_slice_in_dim(values, flag * half, half, 0)


def sum_all(values, axis):
    count = lax.axis_size(axis)
    if count & (count - 1):
        return lax.psum(values, axis)
    step = 1
    while step < count:
        values = values + lax.ppermute(values, axis, [(i, i ^ step) for i in range(count)])
        step *= 2
    return values


def block_places(bits_inner, bits_outer, device):
    places = [(0, 0)]
    for bit in reversed(bits_inner):
        places = places + [(fixed | bit, relative) for fixed, relative in places]
    for bit in bits_outer:
        places = places + [(fixed, relative | bit) for fixed, relative in places]
    mask = sum(bits_outer)
    return [fixed + jnp.bitwise_xor(relative, jnp.bitwise_and(device, mask)) for fixed, relative in places]


def flipped(device, mask, bits):
    for bit in bits:
        if mask & bit:
            device = device + bit - 2 * bit * bit_of(device, bit)
    return device


def index_of(device, bits):
    return sum((bit_of(device, bit) * 2**at for at, bit in enumerate(bits)), 0 * device)


def masks_of(bits):
    masks = [0]
    for bit in bits:
        masks = masks + [mask | bit for mask in masks]
    return masks


class Copies:
    def __init__(self, send_sems, recv_sems):
        self.send_sems, self.recv_sems = send_sems, recv_sems
        self.names = {}
        self.started = []

    def place(self, name):
        return self.names.setdefault(name, len(self.names))

    def start(self, name, pairs, target):
        at = self.place(name)
        for source, destination in pairs:
            copy = pltpu.make_async_remote_copy(
                src_ref=source,
                dst_ref=destination,
                send_sem=self.send_sems.at[at],
                recv_sem=self.recv_sems.at[at],
                device_id=target,
                device_id_type=MESH,
            )
            copy.start()
        self.started.append(at)

    def wait(self, name, whole):
        at = self.place(name)
        pltpu.make_async_copy(whole, whole, self.recv_sems.at[at]).wait()

    def drain(self, name, whole):
        at = self.place(name)
        pltpu.make_async_copy(whole, whole, self.send_sems.at[at]).wait()


def gather_kernel(
    plan,
    hidden_ref,
    upstream_ref,
    weight_ref,
    matrix_ref,
    gain_ref,
    normed_all,
    upstream_all,
    weight_full,
    matrix_full,
    normed_held,
    upstream_held,
    send_sems,
    recv_sems,
    local_sems,
):
    head_bits, outer_bits, ranks = plan
    device = lax.axis_index("dp")
    plane = lax.axis_index("tensor")
    length, model = hidden_ref.shape
    rows = weight_ref.shape[0]
    parts = 2 ** len(head_bits)
    bits = head_bits + outer_bits
    slot_bits = head_bits[::-1]
    group = masks_of(head_bits)
    copies = Copies(send_sems, recv_sems)
    shared = ranks == 2 and any(bit > 1 for bit in head_bits)

    targets = [{"dp": flipped(device, mask, bits)} for mask in group[1:] + outer_bits]
    if shared:
        targets.append({"tensor": 1 - plane})
    barrier = pltpu.get_barrier_semaphore()
    for target in targets:
        pl.semaphore_signal(barrier, inc=1, device_id=target, device_id_type=MESH)
    pl.semaphore_wait(barrier, len(targets))

    def segments(full, ref):
        if full is weight_full:
            keys = KEY_VALUE_HEADS // ranks * HEAD_SIZE
            queries = QUERY_HEADS // ranks * HEAD_SIZE
            return [
                (0, queries // parts, 0),
                (queries, keys // parts, queries // parts),
                (queries + keys, keys // parts, (queries + keys) // parts),
            ]
        return [(0, ref.shape[1] // parts, 0)]

    def own_pairs(full, ref, mask):
        part = index_of(flipped(device, mask, bits), head_bits)
        first = pl.multiple_of(index_of(device, slot_bits) * rows, rows)
        pairs = []
        for start, width, place in segments(full, ref):
            source = ref.at[:, pl.ds(pl.multiple_of(start + part * width, HEAD_SIZE), width)]
            pairs.append((source, full.at[pl.ds(first, rows), pl.ds(place, width)]))
        return pairs

    def item(full, relative, mask):
        slot = index_of(flipped(device, mask, bits), slot_bits)
        first = pl.multiple_of((relative * parts + slot) * rows, rows)
        return full.at[pl.ds(first, rows), :]

    def base_start(name, full, ref):
        for mask in group[:0:-1]:
            copies.start((name, 0, mask), own_pairs(full, ref, mask), {"dp": flipped(device, mask, bits)})

    def outer_start(name, full, relative, mask, first_stage):
        for stage in range(first_stage, len(outer_bits)):
            bit = outer_bits[stage]
            landed = relative + 2**stage
            copies.start(
                (name, landed, mask),
                [(item(full, relative, mask), item(full, landed, mask))],
                {"dp": flipped(device, bit, bits)},
            )

    def arrive(name, full, relative, mask):
        copies.wait((name, relative, mask), item(full, relative, mask))
        stage = relative.bit_length()
        outer_start(name, full, relative, mask, stage)

    def place_own(full, ref, sem):
        pairs = own_pairs(full, ref, 0)
        for source, destination in pairs:
            pltpu.make_async_copy(source, destination, sem).start()

    def own_done(full, sem):
        whole = item(full, 0, 0)
        pltpu.make_async_copy(whole, whole, sem).wait()

    def sequence(full, index):
        return full.at[pl.ds(index * length, length), :]

    half = length // 2

    def half_of(full, index, which):
        first = pl.multiple_of(index * length + which * half, half)
        return full.at[pl.ds(first, half), :]

    token_bits = head_bits[::-1]
    far = [bit for bit in token_bits if bit != 1]
    near = 2 ** len(far) if 1 in token_bits else 0

    def tokens_start(name, full):
        for at, bit in enumerate(far):
            target = {"dp": flipped(device, bit, bits)}
            if shared:
                copies.start(
                    (name, "far"), [(half_of(full, 0, plane), half_of(full, 2**at, plane))], target
                )
            else:
                copies.start((name, "far"), [(sequence(full, 0), sequence(full, 2**at))], target)
        if near:
            copies.start(
                (name, "near"),
                [(sequence(full, 0), sequence(full, near))],
                {"dp": flipped(device, 1, bits)},
            )

    def tokens_far(name, full):
        if not far:
            return
        sibling = {"dp": flipped(device, 1, bits)}
        piece = (lambda index: half_of(full, index, plane)) if shared else (lambda index: sequence(full, index))
        copies.wait((name, "far"), piece(1))
        if shared:
            copies.start((name, "side"), [(piece(1), piece(1))], {"tensor": 1 - plane})
        if near:
            copies.start((name, "cross"), [(piece(1), piece(near + 1))], sibling)

    def tokens_side(name, full):
        if not (far and shared):
            return
        other = half_of(full, 1, 1 - plane)
        copies.wait((name, "side"), other)
        if near:
            copies.start(
                (name, "cross2"),
                [(other, half_of(full, near + 1, 1 - plane))],
                {"dp": flipped(device, 1, bits)},
            )

    def tokens_end(name, full):
        if near:
            copies.wait((name, "near"), sequence(full, near))
            if far:
                piece = half_of(full, near + 1, plane) if shared else sequence(full, near + 1)
                copies.wait((name, "cross"), piece)
                if shared:
                    copies.wait((name, "cross2"), half_of(full, near + 1, 1 - plane))

    relatives = list(range(1, 2 ** len(outer_bits)))
    last = 2 ** (len(outer_bits) - 1)
    early = [relative for relative in relatives if relative < last]
    late = [relative for relative in relatives if relative >= last]

    base_start("w", weight_full, weight_ref)
    place_own(weight_full, weight_ref, local_sems.at[0])
    own_done(weight_full, local_sems.at[0])
    outer_start("w", weight_full, 0, 0, 0)

    inverse = lax.rsqrt(
        jnp.mean(jnp.square(hidden_ref[...].astype(F32)), axis=-1, keepdims=True) + EPSILON
    )
    for relative in range(2 ** len(outer_bits)):
        for slot in range(parts):
            owner = 0 * device
            for at, bit in enumerate(slot_bits):
                owner = owner + bit * ((slot >> at) & 1)
            for at, bit in enumerate(outer_bits):
                flag = bit_of(device, bit)
                owner = owner + bit * (flag + ((relative >> at) & 1) * (1 - 2 * flag))
            source = pl.ds(pl.multiple_of(owner * rows, rows), rows)
            target = pl.ds((relative * parts + slot) * rows, rows)
            piece = hidden_ref[:, source].astype(F32) * inverse * gain_ref[:, source]
            normed_held[:, target] = piece.astype(BF16)
            upstream_held[:, target] = upstream_ref[:, source]
    held_normed = pltpu.make_async_copy(normed_held, sequence(normed_all, 0), local_sems.at[1])
    held_normed.start()
    held_upstream = pltpu.make_async_copy(upstream_held, sequence(upstream_all, 0), local_sems.at[2])
    held_upstream.start()
    for mask in group[1:]:
        if mask == 1:
            arrive("w", weight_full, 0, mask)
    held_normed.wait()
    tokens_start("n", normed_all)
    for mask in group[1:]:
        if mask != 1:
            arrive("w", weight_full, 0, mask)
    base_start("m", matrix_full, matrix_ref)
    place_own(matrix_full, matrix_ref, local_sems.at[3])
    own_done(matrix_full, local_sems.at[3])
    held_upstream.wait()
    for relative in early:
        for mask in group:
            arrive("w", weight_full, relative, mask)
    tokens_far("n", normed_all)
    outer_start("m", matrix_full, 0, 0, 0)
    for mask in group[1:]:
        arrive("m", matrix_full, 0, mask)
    tokens_start("u", upstream_all)
    tokens_side("n", normed_all)
    for relative in late:
        for mask in group:
            arrive("w", weight_full, relative, mask)
    tokens_end("n", normed_all)
    for relative in early:
        for mask in group:
            arrive("m", matrix_full, relative, mask)
    tokens_far("u", upstream_all)
    tokens_side("u", upstream_all)
    for relative in late:
        for mask in group:
            arrive("m", matrix_full, relative, mask)
    tokens_end("u", upstream_all)

    for name, full in (("w", weight_full), ("m", matrix_full)):
        for relative in range(2 ** len(outer_bits)):
            for mask in group:
                if relative or mask:
                    copies.drain((name, relative, mask), item(full, 0, 0))
    for name, full in (("n", normed_all), ("u", upstream_all)):
        if far:
            copies.drain((name, "far"), half_of(full, 0, 0) if shared else sequence(full, 0))
            if shared:
                copies.drain((name, "side"), half_of(full, 0, 0))
        if near:
            copies.drain((name, "near"), sequence(full, 0))
            if far:
                copies.drain((name, "cross"), half_of(full, 0, 0) if shared else sequence(full, 0))
                if shared:
                    copies.drain((name, "cross2"), half_of(full, 0, 0))


def gather_all(plan, hidden_in, upstream, weight, matrix, norm_gain):
    head_bits, outer_bits, _ = plan
    length, model = hidden_in.shape
    parts = 2 ** len(head_bits)
    count = 2 * (2 ** (len(outer_bits) + len(head_bits))) + 12
    anywhere = pl.BlockSpec(memory_space=pl.ANY)
    inside = pl.BlockSpec(memory_space=pltpu.VMEM)
    return pl.pallas_call(
        partial(gather_kernel, plan),
        in_specs=[inside] * 5,
        out_specs=[anywhere] * 4,
        out_shape=[
            jax.ShapeDtypeStruct((parts * length, model), BF16),
            jax.ShapeDtypeStruct((parts * length, model), BF16),
            jax.ShapeDtypeStruct((model, weight.shape[1] // parts), BF16),
            jax.ShapeDtypeStruct((model, matrix.shape[1] // parts), BF16),
        ],
        scratch_shapes=[
            pltpu.VMEM((length, model), BF16),
            pltpu.VMEM((length, model), BF16),
            pltpu.SemaphoreType.DMA((count,)),
            pltpu.SemaphoreType.DMA((count,)),
            pltpu.SemaphoreType.DMA((4,)),
        ],
        compiler_params=pltpu.CompilerParams(
            collective_id=0, has_side_effects=True, vmem_limit_bytes=60 * 1024 * 1024
        ),
        cost_estimate=pl.CostEstimate(
            flops=10**11, bytes_accessed=64 * length * model, transcendentals=length
        ),
        name="gather_all",
    )(hidden_in, upstream, weight, matrix, norm_gain.reshape(1, model))


def row_terms(left, right, first, last):
    return lax.dot_general(
        left[:, first:last], right, (((0,), (0,)), ((), ())), preferred_element_type=F32
    )


def sum_rows(left, right, sent, outer_bits):
    got = swap(sent, outer_bits[-1])
    held = row_terms(left, right, 0, sent.shape[0]) + got.astype(F32)
    for bit in reversed(outer_bits[:-1]):
        half = held.shape[0] // 2
        got = swap(held[half:].astype(BF16), bit)
        held = held[:half] + got.astype(F32)
    return held


def join_heads(held, head_bits, device):
    parts = 2 ** len(head_bits)
    if parts == 1:
        return held[None]
    held = held.astype(BF16).reshape(1, held.shape[0], held.shape[1])
    for bit in head_bits:
        flag = bit_of(device, bit)
        half = held.shape[1] // 2
        kept = lax.dynamic_slice_in_dim(held, flag * half, half, 1)
        sent = lax.dynamic_slice_in_dim(held, (1 - flag) * half, half, 1)
        got = swap(sent, bit)
        held = ordered(flag, kept[None], got[None], 0)
        held = held.reshape(-1, half, held.shape[-1])
    return held


def local(hidden_in, upstream, merged_input_weight, output_matrix, norm_gain, query_gain, key_gain):
    shard_ranks = lax.axis_size("tensor")
    groups = lax.axis_size("dp")
    device = lax.axis_index("dp")
    query_heads = QUERY_HEADS // shard_ranks
    key_heads = KEY_VALUE_HEADS // shard_ranks
    group_width = QUERY_HEADS // KEY_VALUE_HEADS
    length, model = hidden_in.shape
    grad_scale = 1.0 / math.sqrt(groups * length)
    bits = device_bits(groups)
    head_bits = []
    for bit in (1, 4):
        if bit in bits and key_heads % (2 ** (len(head_bits) + 1)) == 0:
            head_bits.append(bit)
    outer_bits = [bit for bit in bits if bit > 2 and bit not in head_bits]
    outer_bits += [bit for bit in bits if bit <= 2 and bit not in head_bits]
    parts = 2 ** len(head_bits)
    places = jnp.stack(block_places(head_bits, outer_bits, device)).astype(jnp.int32)
    part_queries = query_heads // parts
    part_keys = key_heads // parts
    query_columns = part_queries * HEAD_SIZE
    key_columns = part_keys * HEAD_SIZE
    plane = lax.axis_index("tensor")

    rows = merged_input_weight.shape[0]
    q_all, k_all = query_heads * HEAD_SIZE, key_heads * HEAD_SIZE
    chunk = 2 * HEAD_SIZE
    normed_all, upstream_all, weight_full, matrix_full = gather_all(
        (head_bits, outer_bits, shard_ranks),
        hidden_in,
        upstream,
        merged_input_weight,
        output_matrix,
        norm_gain,
    )
    projected = jnp.dot(normed_all, weight_full, preferred_element_type=F32)
    cosine, sine = rope_tables(length, HEAD_SIZE)
    gains = jnp.stack([query_gain, key_gain])
    context_low = attention_forward(projected, gains, cosine, sine, part_keys, group_width)
    context_pieces = [
        context_low[:, at : at + chunk] for at in range(0, query_columns, chunk)
    ]
    context_sent = [
        row_terms(upstream_all, one, model // 2, model).astype(BF16) for one in context_pieces
    ]
    context_sent, projected = lax.optimization_barrier((context_sent, projected))
    output_sums = jnp.concatenate(
        [
            sum_rows(upstream_all, one, sent, outer_bits)
            for one, sent in zip(context_pieces, context_sent)
        ],
        axis=1,
    )
    output_parts = join_heads(output_sums, head_bits, device).astype(F32)
    output_grad = output_parts.transpose(1, 0, 2).reshape(rows, q_all) * grad_scale

    context_gradient = jnp.dot(
        upstream_all, matrix_full, preferred_element_type=F32
    ).astype(BF16)
    grad_projected, head_sums = attention_backward(
        projected, context_gradient, gains, cosine, sine, part_keys, group_width
    )

    share = lax.dot_general(
        grad_projected, weight_full, (((1,), (1,)), ((), ())), preferred_element_type=F32
    ).astype(BF16)
    grad_pieces = [
        grad_projected[:, at : at + chunk] for at in range(0, grad_projected.shape[1], chunk)
    ]
    input_sums = jnp.concatenate(
        [
            sum_rows(
                normed_all,
                one,
                row_terms(normed_all, one, model // 2, model).astype(BF16),
                outer_bits,
            )
            for one in grad_pieces
        ],
        axis=1,
    )
    input_parts = join_heads(input_sums, head_bits, device).astype(F32) * grad_scale
    input_grad = jnp.concatenate(
        [
            input_parts[:, :, :query_columns].transpose(1, 0, 2).reshape(rows, q_all),
            input_parts[:, :, query_columns : query_columns + key_columns]
            .transpose(1, 0, 2)
            .reshape(rows, k_all),
            input_parts[:, :, query_columns + key_columns :].transpose(1, 0, 2).reshape(rows, k_all),
        ],
        axis=1,
    )

    held = [share[i * length : (i + 1) * length] for i in range(parts)]
    for bit in head_bits:
        half = len(held) // 2
        if bit == 1 or shard_ranks != 2:
            got = [swap(one.astype(BF16), bit) for one in held[half:]]
            held = [one.astype(F32) + other.astype(F32) for one, other in zip(held[:half], got)]
        else:
            fresh = []
            for one, away in zip(held[:half], held[half:]):
                mine = half_rows(away, plane).astype(F32)
                got = swap_tensor(half_rows(away, 1 - plane).astype(BF16))
                back = swap((mine + got.astype(F32)).astype(BF16), bit)
                zero = jnp.zeros_like(back)
                spread = jnp.where(
                    plane == 0,
                    jnp.concatenate([back, zero], 0),
                    jnp.concatenate([zero, back], 0),
                )
                fresh.append(one.astype(F32) + spread.astype(F32))
            held = fresh
    partial_normed = held[0].astype(BF16)
    shares = [partial_normed] + [
        lax.ppermute(
            partial_normed, "tensor", [(i, (i + shift) % shard_ranks) for i in range(shard_ranks)]
        )
        for shift in range(1, shard_ranks)
    ]
    hidden_grad, gain_part = leave(places, hidden_in, upstream, norm_gain, shares)
    sums = jnp.concatenate([gain_part * (1.0 / shard_ranks), head_sums[0], head_sums[1]])
    sums = sum_all(sum_all(sums, "tensor"), "dp")
    gain_sum, query_sum, key_sum = jnp.split(sums, [model, model + HEAD_SIZE])
    return (
        hidden_grad,
        input_grad,
        output_grad,
        gain_sum * grad_scale,
        query_sum * grad_scale,
        key_sum * grad_scale,
    )


def solution(mesh):
    in_specs = (P("dp", None), P("dp", None), P("dp", "tensor"), P("dp", "tensor"), P(), P(), P())
    out_specs = (P("dp", None), P("dp", "tensor"), P("dp", "tensor"), P(), P(), P())
    return jax.shard_map(local, mesh=mesh, in_specs=in_specs, out_specs=out_specs, check_vma=False)
```

```python
from functools import partial
import math

import jax
import jax.numpy as jnp
from jax import lax
from jax.experimental import pallas as pl
from jax.experimental.pallas import tpu as pltpu
from jax.sharding import PartitionSpec as P

QUERY_HEADS = 32
KEY_VALUE_HEADS = 8
HEAD_SIZE = 128


EPSILON = 1e-06
ROPE_BASE = 1000000.0
F32 = jnp.float32
BF16 = jnp.bfloat16
ROW_BLOCK = 128
MESH = pl.DeviceIdType.MESH


def rope_tables(length, columns):
    half_width = columns // 2
    exponent = jnp.arange(half_width, dtype=jnp.float32) * (2.0 / columns)
    frequency = jnp.exp(-exponent * math.log(ROPE_BASE))
    places = jnp.arange(length, dtype=jnp.float32)
    angles = places[:, None] * frequency[None, :]
    cosine, sine = jnp.cos(angles), jnp.sin(angles)
    return (
        jnp.concatenate([cosine, cosine], axis=1),
        jnp.concatenate([-sine, sine], axis=1),
    )


def call_params(vmem_mib):
    return pltpu.CompilerParams(
        dimension_semantics=("arbitrary",), vmem_limit_bytes=vmem_mib * 1024 * 1024
    )


def leave_kernel(places_ref, hidden_ref, upstream_ref, gain_ref, *rest):
    *shares, grad_ref, gain_grad_ref, natural = rest
    count = places_ref.shape[0]
    width = hidden_ref.shape[1] // count
    for at in range(count):
        target = pl.ds(pl.multiple_of(places_ref[at] * width, width), width)
        source = slice(at * width, (at + 1) * width)
        total = shares[0][:, source].astype(F32)
        for other in shares[1:]:
            total = total + other[:, source].astype(F32)
        natural[:, target] = total
    states = hidden_ref[...].astype(F32)
    inverse = lax.rsqrt(jnp.mean(states * states, axis=-1, keepdims=True) + EPSILON)
    unit = states * inverse
    part = jnp.sum(natural[...] * unit, axis=0, keepdims=True)

    @pl.when(pl.program_id(0) == 0)
    def _():
        gain_grad_ref[...] = part

    @pl.when(pl.program_id(0) != 0)
    def _():
        gain_grad_ref[...] += part

    scaled = natural[...] * gain_ref[...]
    mean = jnp.mean(scaled * unit, axis=-1, keepdims=True)
    grad = inverse * (scaled - unit * mean)
    grad_ref[...] = (upstream_ref[...].astype(F32) + grad).astype(BF16)


def leave(places, hidden_in, upstream, norm_gain, shares):
    length, model = hidden_in.shape
    block = min(length, ROW_BLOCK)
    whole = pl.BlockSpec((block, model), lambda i, places: (i, 0))
    line = pl.BlockSpec((1, model), lambda i, places: (0, 0))
    hidden_grad, gain_part = pl.pallas_call(
        leave_kernel,
        grid_spec=pltpu.PrefetchScalarGridSpec(
            num_scalar_prefetch=1,
            grid=(length // block,),
            in_specs=[whole, whole, line] + [whole] * len(shares),
            out_specs=[whole, line],
            scratch_shapes=[pltpu.VMEM((block, model), F32)],
        ),
        out_shape=[
            jax.ShapeDtypeStruct((length, model), BF16),
            jax.ShapeDtypeStruct((1, model), F32),
        ],
        compiler_params=call_params(40),
        cost_estimate=pl.CostEstimate(
            flops=12 * length * model,
            bytes_accessed=(6 + 2 * len(shares)) * length * model,
            transcendentals=length,
        ),
        name="leave",
    )(places, hidden_in, upstream, norm_gain.reshape(1, model), *shares)
    return hidden_grad, gain_part[0]


def turn(values):
    return pltpu.roll(values, HEAD_SIZE // 2, 1)


def head_states(raw, gain, cosine, sine):
    inverse = lax.rsqrt(jnp.mean(raw * raw, axis=-1, keepdims=True) + EPSILON)
    normed = raw * inverse * gain
    return (normed * cosine + turn(normed) * sine).astype(BF16)


def head_back(grad, raw, gain, cosine, sine):
    inverse = lax.rsqrt(jnp.mean(raw * raw, axis=-1, keepdims=True) + EPSILON)
    unit = raw * inverse
    grad_normed = grad * cosine + turn(grad * sine)
    part = jnp.sum(grad_normed * unit, axis=0, keepdims=True)
    scaled = grad_normed * gain
    mean = jnp.mean(scaled * unit, axis=-1, keepdims=True)
    return inverse * (scaled - unit * mean), part


def columns_of(index):
    return slice(index * HEAD_SIZE, (index + 1) * HEAD_SIZE)


def matmul(left, right, contract):
    return lax.dot_general(left, right, ((contract[:1], contract[1:]), ((), ())), preferred_element_type=F32)


def block_probs(queries, keys, tile, width, scale):
    scores = matmul(queries, keys, (1, 1)) * scale
    height = scores.shape[0]
    at_row = lax.rem(lax.broadcasted_iota(jnp.int32, (height, width), 0), tile) + (width - tile)
    causal = at_row >= lax.broadcasted_iota(jnp.int32, (height, width), 1)
    raised = jnp.where(causal, jnp.exp(scores), 0.0)
    return raised / jnp.sum(raised, axis=-1, keepdims=True)


def forward_kernel(heads, group, tile, raw_ref, gains_ref, cosine_ref, sine_ref, context_ref):
    length = raw_ref.shape[0]
    query_total = heads * group
    scale = 1.0 / math.sqrt(HEAD_SIZE)
    for head in range(heads):
        keys = head_states(
            raw_ref[:, columns_of(query_total + head)], gains_ref[1:2], cosine_ref[...], sine_ref[...]
        )
        values = raw_ref[:, columns_of(query_total + heads + head)].astype(BF16)
        for start in range(0, length, tile):
            rows = slice(start, start + tile)
            width = start + tile
            queries = jnp.concatenate(
                [
                    head_states(
                        raw_ref[rows, columns_of(head * group + one)],
                        gains_ref[0:1],
                        cosine_ref[rows],
                        sine_ref[rows],
                    )
                    for one in range(group)
                ],
                axis=0,
            )
            probs = block_probs(queries, keys[:width], tile, width, scale)
            context = matmul(probs.astype(BF16), values[:width], (1, 0)).astype(BF16)
            for one in range(group):
                context_ref[rows, columns_of(head * group + one)] = context[one * tile : (one + 1) * tile]


def backward_kernel(
    heads, group, tile, raw_ref, grad_ref, gains_ref, cosine_ref, sine_ref, out_ref, sums_ref, step
):
    length = raw_ref.shape[0]
    query_total = heads * group
    scale = 1.0 / math.sqrt(HEAD_SIZE)
    query_sum = jnp.zeros((1, HEAD_SIZE), F32)
    key_sum = jnp.zeros((1, HEAD_SIZE), F32)
    for head in range(heads):
        raw_keys = raw_ref[:, columns_of(query_total + head)]
        keys = head_states(raw_keys, gains_ref[1:2], cosine_ref[...], sine_ref[...])
        values = raw_ref[:, columns_of(query_total + heads + head)].astype(BF16)
        grad_keys = [jnp.zeros((tile, HEAD_SIZE), F32) for _ in range(length // tile)]
        grad_values = [jnp.zeros((tile, HEAD_SIZE), F32) for _ in range(length // tile)]
        for start in range(0, length, tile):
            rows = slice(start, start + tile)
            width = start + tile
            raw = jnp.concatenate(
                [raw_ref[rows, columns_of(head * group + one)] for one in range(group)], axis=0
            )
            cosine = jnp.concatenate([cosine_ref[rows]] * group, axis=0)
            sine = jnp.concatenate([sine_ref[rows]] * group, axis=0)
            queries = head_states(raw, gains_ref[0:1], cosine, sine)
            probs = block_probs(queries, keys[:width], tile, width, scale)
            probs_low = probs.astype(BF16)
            context_grad = jnp.concatenate(
                [grad_ref[rows, columns_of(head * group + one)] for one in range(group)], axis=0
            )
            grad_probs = matmul(context_grad, values[:width], (1, 1))
            centre = jnp.sum(probs * grad_probs, axis=-1, keepdims=True)
            grad_scores = (probs * (grad_probs - centre) * scale).astype(BF16)
            part_values = matmul(probs_low, context_grad, (0, 0))
            part_keys = matmul(grad_scores, queries, (0, 0))
            for at in range(width // tile):
                piece = slice(at * tile, (at + 1) * tile)
                grad_values[at] = grad_values[at] + part_values[piece]
                grad_keys[at] = grad_keys[at] + part_keys[piece]
            grad_queries = matmul(grad_scores, keys[:width], (1, 0))
            grad_raw, part = head_back(grad_queries, raw, gains_ref[0:1], cosine, sine)
            query_sum = query_sum + part
            grad_raw = grad_raw.astype(BF16)
            for one in range(group):
                out_ref[rows, columns_of(head * group + one)] = grad_raw[one * tile : (one + 1) * tile]
        grad_raw, part = head_back(
            jnp.concatenate(grad_keys, axis=0), raw_keys, gains_ref[1:2], cosine_ref[...], sine_ref[...]
        )
        key_sum = key_sum + part
        out_ref[:, columns_of(query_total + head)] = grad_raw.astype(BF16)
        out_ref[:, columns_of(query_total + heads + head)] = jnp.concatenate(
            grad_values, axis=0
        ).astype(BF16)
    sums = jnp.concatenate([query_sum, key_sum], axis=0)

    @pl.when(step == 0)
    def _():
        sums_ref[...] = sums

    @pl.when(step != 0)
    def _():
        sums_ref[...] += sums


def attention_specs(length, heads, group):
    return (
        pl.BlockSpec((length, (heads * group + 2 * heads) * HEAD_SIZE), lambda i: (i, 0)),
        pl.BlockSpec((length, heads * group * HEAD_SIZE), lambda i: (i, 0)),
        pl.BlockSpec((2, HEAD_SIZE), lambda i: (0, 0)),
        pl.BlockSpec((length, HEAD_SIZE), lambda i: (0, 0)),
    )


def attention_forward(raw, gains, cosine, sine, heads, group):
    length = cosine.shape[0]
    sequences = raw.shape[0] // length
    raw_spec, head_spec, gain_spec, table_spec = attention_specs(length, heads, group)
    pairs = sequences * heads * group * length * length
    return pl.pallas_call(
        partial(forward_kernel, heads, group, min(length, ROW_BLOCK)),
        grid=(sequences,),
        in_specs=[raw_spec, gain_spec, table_spec, table_spec],
        out_specs=head_spec,
        out_shape=jax.ShapeDtypeStruct((raw.shape[0], heads * group * HEAD_SIZE), BF16),
        compiler_params=call_params(40),
        cost_estimate=pl.CostEstimate(
            flops=8 * pairs * HEAD_SIZE, bytes_accessed=raw.size * 6, transcendentals=pairs
        ),
        name="attention_forward",
    )(raw, gains, cosine, sine)


def device_bits(count):
    bits = []
    bit = 1
    while bit < count:
        bits.append(bit)
        bit *= 2
    return bits


def bit_of(index, bit):
    return (index // bit) % 2


def sum_all(values, axis):
    count = lax.axis_size(axis)
    if count & (count - 1):
        return lax.psum(values, axis)
    step = 1
    while step < count:
        values = values + lax.ppermute(values, axis, [(i, i ^ step) for i in range(count)])
        step *= 2
    return values


def block_places(bits_inner, bits_outer, device):
    places = [(0, 0)]
    for bit in reversed(bits_inner):
        places = places + [(fixed | bit, relative) for fixed, relative in places]
    for bit in bits_outer:
        places = places + [(fixed, relative | bit) for fixed, relative in places]
    mask = sum(bits_outer)
    return [fixed + jnp.bitwise_xor(relative, jnp.bitwise_and(device, mask)) for fixed, relative in places]


def flipped(device, mask, bits):
    for bit in bits:
        if mask & bit:
            device = device + bit - 2 * bit * bit_of(device, bit)
    return device


def index_of(device, bits):
    return sum((bit_of(device, bit) * 2**at for at, bit in enumerate(bits)), 0 * device)


def masks_of(bits):
    masks = [0]
    for bit in bits:
        masks = masks + [mask | bit for mask in masks]
    return masks


class Copies:
    def __init__(self, send_sems, recv_sems):
        self.send_sems, self.recv_sems = send_sems, recv_sems
        self.names = {}
        self.started = []

    def place(self, name):
        return self.names.setdefault(name, len(self.names))

    def start(self, name, pairs, target):
        at = self.place(name)
        for source, destination in pairs:
            copy = pltpu.make_async_remote_copy(
                src_ref=source,
                dst_ref=destination,
                send_sem=self.send_sems.at[at],
                recv_sem=self.recv_sems.at[at],
                device_id=target,
                device_id_type=MESH,
            )
            copy.start()
        self.started.append(at)

    def wait(self, name, whole):
        at = self.place(name)
        pltpu.make_async_copy(whole, whole, self.recv_sems.at[at]).wait()

    def drain(self, name, whole):
        at = self.place(name)
        pltpu.make_async_copy(whole, whole, self.send_sems.at[at]).wait()


def gather_kernel(
    plan,
    hidden_ref,
    upstream_ref,
    weight_ref,
    matrix_ref,
    gain_ref,
    normed_all,
    upstream_all,
    weight_full,
    matrix_full,
    weight_other,
    normed_held,
    upstream_held,
    send_sems,
    recv_sems,
    local_sems,
):
    head_bits, outer_bits, ranks = plan
    device = lax.axis_index("dp")
    plane = lax.axis_index("tensor")
    length, model = hidden_ref.shape
    rows = weight_ref.shape[0]
    parts = 2 ** len(head_bits)
    bits = head_bits + outer_bits
    slot_bits = head_bits[::-1]
    group = masks_of(head_bits)
    copies = Copies(send_sems, recv_sems)
    shared = ranks == 2 and any(bit > 1 for bit in head_bits)

    targets = [{"dp": flipped(device, mask, bits)} for mask in group[1:] + outer_bits]
    if shared:
        targets.append({"tensor": 1 - plane})
    barrier = pltpu.get_barrier_semaphore()
    for target in targets:
        pl.semaphore_signal(barrier, inc=1, device_id=target, device_id_type=MESH)
    pl.semaphore_wait(barrier, len(targets))

    def segments(full, ref):
        if full is weight_full:
            keys = KEY_VALUE_HEADS // ranks * HEAD_SIZE
            queries = QUERY_HEADS // ranks * HEAD_SIZE
            return [
                (0, queries // parts, 0),
                (queries, keys // parts, queries // parts),
                (queries + keys, keys // parts, (queries + keys) // parts),
            ]
        return [(0, ref.shape[1] // parts, 0)]

    def own_pairs(full, ref, mask):
        part = index_of(flipped(device, mask, bits), head_bits)
        first = pl.multiple_of(index_of(device, slot_bits) * rows, rows)
        pairs = []
        for start, width, place in segments(full, ref):
            source = ref.at[:, pl.ds(pl.multiple_of(start + part * width, HEAD_SIZE), width)]
            pairs.append((source, full.at[pl.ds(first, rows), pl.ds(place, width)]))
        return pairs

    def item(full, relative, mask):
        slot = index_of(flipped(device, mask, bits), slot_bits)
        first = pl.multiple_of((relative * parts + slot) * rows, rows)
        return full.at[pl.ds(first, rows), :]

    def base_start(name, full, ref):
        for mask in group[:0:-1]:
            copies.start((name, 0, mask), own_pairs(full, ref, mask), {"dp": flipped(device, mask, bits)})

    def outer_start(name, full, relative, mask, first_stage):
        for stage in range(first_stage, len(outer_bits)):
            bit = outer_bits[stage]
            landed = relative + 2**stage
            copies.start(
                (name, landed, mask),
                [(item(full, relative, mask), item(full, landed, mask))],
                {"dp": flipped(device, bit, bits)},
            )
        if full is weight_full and parts > 1:
            copies.start(
                ("x", relative, mask),
                [(item(full, relative, mask), item(weight_other, relative, mask))],
                {"dp": flipped(device, 1, bits)},
            )

    def arrive(name, full, relative, mask):
        copies.wait((name, relative, mask), item(full, relative, mask))
        stage = relative.bit_length()
        outer_start(name, full, relative, mask, stage)

    def place_own(full, ref, sem):
        pairs = own_pairs(full, ref, 0)
        for source, destination in pairs:
            pltpu.make_async_copy(source, destination, sem).start()

    def own_done(full, sem):
        whole = item(full, 0, 0)
        pltpu.make_async_copy(whole, whole, sem).wait()

    def sequence(full, index):
        return full.at[pl.ds(index * length, length), :]

    half = length // 2

    def half_of(full, index, which):
        first = pl.multiple_of(index * length + which * half, half)
        return full.at[pl.ds(first, half), :]

    token_bits = head_bits[::-1]
    far = [bit for bit in token_bits if bit != 1]
    near = 2 ** len(far) if 1 in token_bits else 0

    def tokens_start(name, full):
        for at, bit in enumerate(far):
            target = {"dp": flipped(device, bit, bits)}
            if shared:
                copies.start(
                    (name, "far"), [(half_of(full, 0, plane), half_of(full, 2**at, plane))], target
                )
            else:
                copies.start((name, "far"), [(sequence(full, 0), sequence(full, 2**at))], target)
        if near:
            copies.start(
                (name, "near"),
                [(sequence(full, 0), sequence(full, near))],
                {"dp": flipped(device, 1, bits)},
            )

    def tokens_far(name, full):
        if not far:
            return
        sibling = {"dp": flipped(device, 1, bits)}
        piece = (lambda index: half_of(full, index, plane)) if shared else (lambda index: sequence(full, index))
        copies.wait((name, "far"), piece(1))
        if shared:
            copies.start((name, "side"), [(piece(1), piece(1))], {"tensor": 1 - plane})
        if near:
            copies.start((name, "cross"), [(piece(1), piece(near + 1))], sibling)

    def tokens_side(name, full):
        if not (far and shared):
            return
        other = half_of(full, 1, 1 - plane)
        copies.wait((name, "side"), other)
        if near:
            copies.start(
                (name, "cross2"),
                [(other, half_of(full, near + 1, 1 - plane))],
                {"dp": flipped(device, 1, bits)},
            )

    def tokens_end(name, full):
        if near:
            copies.wait((name, "near"), sequence(full, near))
            if far:
                piece = half_of(full, near + 1, plane) if shared else sequence(full, near + 1)
                copies.wait((name, "cross"), piece)
                if shared:
                    copies.wait((name, "cross2"), half_of(full, near + 1, 1 - plane))

    relatives = list(range(1, 2 ** len(outer_bits)))
    last = 2 ** (len(outer_bits) - 1)
    early = [relative for relative in relatives if relative < last]
    late = [relative for relative in relatives if relative >= last]

    base_start("w", weight_full, weight_ref)
    place_own(weight_full, weight_ref, local_sems.at[0])
    own_done(weight_full, local_sems.at[0])
    outer_start("w", weight_full, 0, 0, 0)

    inverse = lax.rsqrt(
        jnp.mean(jnp.square(hidden_ref[...].astype(F32)), axis=-1, keepdims=True) + EPSILON
    )
    for relative in range(2 ** len(outer_bits)):
        for slot in range(parts):
            owner = 0 * device
            for at, bit in enumerate(slot_bits):
                owner = owner + bit * ((slot >> at) & 1)
            for at, bit in enumerate(outer_bits):
                flag = bit_of(device, bit)
                owner = owner + bit * (flag + ((relative >> at) & 1) * (1 - 2 * flag))
            source = pl.ds(pl.multiple_of(owner * rows, rows), rows)
            target = pl.ds((relative * parts + slot) * rows, rows)
            piece = hidden_ref[:, source].astype(F32) * inverse * gain_ref[:, source]
            normed_held[:, target] = piece.astype(BF16)
            upstream_held[:, target] = upstream_ref[:, source]
    held_normed = pltpu.make_async_copy(normed_held, sequence(normed_all, 0), local_sems.at[1])
    held_normed.start()
    held_upstream = pltpu.make_async_copy(upstream_held, sequence(upstream_all, 0), local_sems.at[2])
    held_upstream.start()
    for mask in group[1:]:
        if mask == 1:
            arrive("w", weight_full, 0, mask)
    held_normed.wait()
    tokens_start("n", normed_all)
    for mask in group[1:]:
        if mask != 1:
            arrive("w", weight_full, 0, mask)
    base_start("m", matrix_full, matrix_ref)
    place_own(matrix_full, matrix_ref, local_sems.at[3])
    own_done(matrix_full, local_sems.at[3])
    held_upstream.wait()
    for relative in early:
        for mask in group:
            arrive("w", weight_full, relative, mask)
    tokens_far("n", normed_all)
    outer_start("m", matrix_full, 0, 0, 0)
    for mask in group[1:]:
        arrive("m", matrix_full, 0, mask)
    tokens_start("u", upstream_all)
    tokens_side("n", normed_all)
    for relative in late:
        for mask in group:
            arrive("w", weight_full, relative, mask)
    tokens_end("n", normed_all)
    for relative in early:
        for mask in group:
            arrive("m", matrix_full, relative, mask)
    tokens_far("u", upstream_all)
    tokens_side("u", upstream_all)
    for relative in late:
        for mask in group:
            arrive("m", matrix_full, relative, mask)
    tokens_end("u", upstream_all)
    if parts > 1:
        for relative in range(2 ** len(outer_bits)):
            for mask in group:
                copies.wait(("x", relative, mask), item(weight_other, relative, mask))
                copies.drain(("x", relative, mask), item(weight_other, relative, mask))

    for name, full in (("w", weight_full), ("m", matrix_full)):
        for relative in range(2 ** len(outer_bits)):
            for mask in group:
                if relative or mask:
                    copies.drain((name, relative, mask), item(full, 0, 0))
    for name, full in (("n", normed_all), ("u", upstream_all)):
        if far:
            copies.drain((name, "far"), half_of(full, 0, 0) if shared else sequence(full, 0))
            if shared:
                copies.drain((name, "side"), half_of(full, 0, 0))
        if near:
            copies.drain((name, "near"), sequence(full, 0))
            if far:
                copies.drain((name, "cross"), half_of(full, 0, 0) if shared else sequence(full, 0))
                if shared:
                    copies.drain((name, "cross2"), half_of(full, 0, 0))


def gather_all(plan, hidden_in, upstream, weight, matrix, norm_gain):
    head_bits, outer_bits, _ = plan
    length, model = hidden_in.shape
    parts = 2 ** len(head_bits)
    count = 3 * (2 ** (len(outer_bits) + len(head_bits))) + 12
    anywhere = pl.BlockSpec(memory_space=pl.ANY)
    inside = pl.BlockSpec(memory_space=pltpu.VMEM)
    return pl.pallas_call(
        partial(gather_kernel, plan),
        in_specs=[inside] * 5,
        out_specs=[anywhere] * 5,
        out_shape=[
            jax.ShapeDtypeStruct((parts * length, model), BF16),
            jax.ShapeDtypeStruct((parts * length, model), BF16),
            jax.ShapeDtypeStruct((model, weight.shape[1] // parts), BF16),
            jax.ShapeDtypeStruct((model, matrix.shape[1] // parts), BF16),
            jax.ShapeDtypeStruct((model if parts > 1 else 16, weight.shape[1] // parts), BF16),
        ],
        scratch_shapes=[
            pltpu.VMEM((length, model), BF16),
            pltpu.VMEM((length, model), BF16),
            pltpu.SemaphoreType.DMA((count,)),
            pltpu.SemaphoreType.DMA((count,)),
            pltpu.SemaphoreType.DMA((4,)),
        ],
        compiler_params=pltpu.CompilerParams(
            collective_id=0, has_side_effects=True, vmem_limit_bytes=60 * 1024 * 1024
        ),
        cost_estimate=pl.CostEstimate(
            flops=10**11, bytes_accessed=64 * length * model, transcendentals=length
        ),
        name="gather_all",
    )(hidden_in, upstream, weight, matrix, norm_gain.reshape(1, model))


def scatter_kernel(
    plan,
    upstream_all,
    normed_all,
    weight_full,
    weight_other,
    context_ref,
    context_grad_ref,
    raw_ref,
    gains_ref,
    cosine_ref,
    sine_ref,
    output_ref,
    input_ref,
    total_ref,
    sums_ref,
    grad_ref,
    grad_other,
    left_held,
    weight_held,
    output_stage,
    output_landed,
    input_stage,
    input_landed,
    output_last,
    output_final,
    input_last,
    input_final,
    share_block,
    share_sent,
    share_got,
    share_own,
    share_far,
    send_sems,
    recv_sems,
    left_sems,
    weight_sems,
):
    head_bits, outer_bits, ranks, heads, group = plan
    device = lax.axis_index("dp")
    plane = lax.axis_index("tensor")
    parts = 2 ** len(head_bits)
    relatives = 2 ** len(outer_bits)
    length = cosine_ref.shape[0]
    model = weight_full.shape[0]
    rows = model // (parts * relatives)
    bits = head_bits + outer_bits
    slot_bits = head_bits[::-1]
    masks = masks_of(head_bits)
    scale = 1.0 / math.sqrt(lax.axis_size("dp") * length)
    copies = Copies(send_sems, recv_sems)

    targets = [{"dp": flipped(device, mask, bits)} for mask in masks[1:] + outer_bits]
    if parts > 1:
        targets.append({"tensor": 1 - plane})
    barrier = pltpu.get_barrier_semaphore()
    for target in targets:
        pl.semaphore_signal(barrier, inc=1, device_id=target, device_id_type=MESH)
    pl.semaphore_wait(barrier, len(targets))

    kinds = {
        "o": (upstream_all, context_ref, output_stage, output_landed, output_last, output_final, output_ref),
        "g": (normed_all, grad_ref, input_stage, input_landed, input_last, input_final, input_ref),
    }
    blocks = {"o": 0, "g": (relatives - 1) * parts + parts - 1}
    block_count = (relatives - 1) * parts + parts - 1

    def partner(mask_index):
        target, slot = device, 0 * device
        for at, bit in enumerate(head_bits):
            change = (mask_index // 2**at) % 2
            flag = bit_of(device, bit)
            target = target + bit * change * (1 - 2 * flag)
            slot = slot + 2 ** slot_bits.index(bit) * (flag + change - 2 * flag * change)
        return target, slot

    def left_copy(kind, relative, index):
        _, slot = partner(index)
        first = pl.multiple_of((relative * parts + slot) * rows, rows)
        return pltpu.make_async_copy(
            kinds[kind][0].at[:, pl.ds(first, rows)],
            left_held.at[lax.rem(index, 2)],
            left_sems.at[lax.rem(index, 2)],
        )

    def remote(kind, at, source, destination, target):
        return pltpu.make_async_remote_copy(
            src_ref=source,
            dst_ref=destination,
            send_sem=send_sems.at[blocks[kind] + at],
            recv_sem=recv_sems.at[blocks[kind] + at],
            device_id=target,
            device_id_type=MESH,
        )

    def handle(kind, relative, index):
        _, right, stage, landed, last, final, result = kinds[kind]

        @pl.when(index + 1 < parts)
        def _():
            left_copy(kind, relative, index + 1).start()

        left_copy(kind, relative, index).wait()
        total = matmul(left_held[lax.rem(index, 2)], right[...], (0, 0))
        top = relative.bit_length()
        for later in range(top, len(outer_bits)):
            source = relative + 2**later
            at = (source - 1) * parts + index
            piece = landed.at[at]
            pltpu.make_async_copy(piece, piece, recv_sems.at[blocks[kind] + at]).wait()
            total = total + piece[...].astype(F32)
        if relative:
            at = (relative - 1) * parts + index
            stage[at] = total.astype(BF16)
            target = {"dp": flipped(device, outer_bits[top - 1], bits)}
            remote(kind, at, stage.at[at], landed.at[at], target).start()
        else:
            last[index] = total.astype(BF16)

            @pl.when(index > 0)
            def _():
                target, _ = partner(index)
                at = (relatives - 1) * parts + index - 1
                remote(kind, at, last.at[index], final.at[index - 1], {"dp": target}).start()

    def process(kind, relative):
        left_copy(kind, relative, 0).start()

        def body(index, carry):
            handle(kind, relative, index)
            return carry

        lax.fori_loop(0, parts, body, 0)

    for relative in range(relatives - 1, 1, -1):
        process("o", relative)

    left_copy("o", 1, 0).start()

    def sequence_step(index, carry):
        span = pl.ds(pl.multiple_of(index * length, length), length)
        backward_kernel(
            heads,
            group,
            min(length, ROW_BLOCK),
            raw_ref.at[span],
            context_grad_ref.at[span],
            gains_ref,
            cosine_ref,
            sine_ref,
            grad_ref.at[span],
            sums_ref,
            index,
        )
        handle("o", 1, index)
        return carry

    lax.fori_loop(0, parts, sequence_step, 0)

    if parts > 1:
        near = (parts // 2) * length
        copies.names = {("skip", at): at for at in range(2 * block_count)}
        copies.start(
            "grad",
            [(grad_ref.at[pl.ds(near, near)], grad_other)],
            {"dp": flipped(device, 1, bits)},
        )
    for relative in range(relatives - 1, 1, -1):
        process("g", relative)

    width = weight_held.shape[2]
    weight_blocks = model // width

    def weight_copies(index):
        slot = lax.rem(index, 2)
        span = pl.ds(pl.multiple_of(index * width, width), width)
        pairs = [(weight_full, 0)] + ([(weight_other, 1)] if parts > 1 else [])
        return [
            pltpu.make_async_copy(full.at[span], weight_held.at[slot, at], weight_sems.at[slot, at])
            for full, at in pairs
        ]

    half = length // 2
    mine = pl.ds(pl.multiple_of(plane % 2 * half, half), half)
    theirs = pl.ds(pl.multiple_of((1 - plane % 2) * half, half), half)
    taken = (parts // 2) * length if parts > 1 else length

    for copy in weight_copies(0):
        copy.start()
    if parts > 1:
        copies.wait("grad", grad_other)

    def weight_step(index, carry):
        @pl.when(index + 1 < weight_blocks)
        def _():
            for copy in weight_copies(index + 1):
                copy.start()

        for copy in weight_copies(index):
            copy.wait()
        slot = lax.rem(index, 2)
        span = pl.ds(pl.multiple_of(index * width, width), width)
        share = matmul(grad_ref[0:taken], weight_held[slot, 0], (1, 1))
        if parts > 1:
            share = share + matmul(grad_other[...], weight_held[slot, 1], (1, 1))
            share_block[...] = share
            far_mine = pl.ds(pl.multiple_of(length + plane % 2 * half, half), half)
            far_theirs = pl.ds(pl.multiple_of(length + (1 - plane % 2) * half, half), half)
            share_far[:, span] = share_block[far_mine, :].astype(BF16)
            share_sent[0, :, span] = share_block[far_theirs, :].astype(BF16)
            share_own[:, span] = share_block[mine, :].astype(BF16)
            share_sent[1, :, span] = share_block[theirs, :].astype(BF16)
        else:
            total_ref[:, span] = share.astype(BF16)
        return carry

    lax.fori_loop(0, weight_blocks, weight_step, 0)
    side = {"tensor": 1 - plane}
    if parts > 1:
        for at in range(2):
            copies.start(("side", at), [(share_sent.at[at], share_got.at[at])], side)
    process("o", 0)
    if relatives > 1:
        process("g", 1)
    if parts > 1:
        across = {"dp": flipped(device, 4, bits)}
        copies.wait(("side", 0), share_got.at[0])
        share_far[...] = (share_far[...].astype(F32) + share_got[0].astype(F32)).astype(BF16)
        copies.start("across", [(share_far, share_got.at[2])], across)
        copies.wait(("side", 1), share_got.at[1])
        copies.wait("across", share_got.at[2])
        share_own[...] = (
            share_own[...].astype(F32) + share_got[1].astype(F32) + share_got[2].astype(F32)
        ).astype(BF16)
        total_ref[mine, :] = share_own[...]
        copies.start("back", [(share_own, total_ref.at[mine])], side)
    process("g", 0)

    def finish(kind):
        _, _, stage, _, last, final, result = kinds[kind]
        if kind == "o":
            spans = [(0, heads * group * HEAD_SIZE, 0)]
        else:
            query, key = heads * group * HEAD_SIZE, heads * HEAD_SIZE
            spans = [
                (0, query, 0),
                (query, key, parts * query),
                (query + key, key, parts * (query + key)),
            ]
        for index in range(parts):
            if index:
                at = (relatives - 1) * parts + index - 1
                piece = final.at[index - 1]
                pltpu.make_async_copy(piece, piece, recv_sems.at[blocks[kind] + at]).wait()
            values = (last[0] if index == 0 else final[index - 1]).astype(F32) * scale
            part = index_of(flipped(device, masks[index], bits), head_bits)
            for start, columns, place in spans:
                result[:, pl.ds(pl.multiple_of(place + part * columns, HEAD_SIZE), columns)] = values[
                    :, start : start + columns
                ]

    finish("o")
    finish("g")
    if parts > 1:
        copies.wait("back", total_ref.at[theirs])

    for kind in ("o", "g"):
        _, _, stage, _, last, _, _ = kinds[kind]
        for at in range(block_count):
            piece = stage.at[0]
            pltpu.make_async_copy(piece, piece, send_sems.at[blocks[kind] + at]).wait()
    if parts > 1:
        copies.drain("grad", grad_other)
        copies.drain(("side", 0), share_far)
        copies.drain(("side", 1), share_far)
        copies.drain("across", share_far)
        copies.drain("back", share_own)


def scatter_all(plan, upstream_all, normed_all, weight_full, weight_other, context, context_grad, raw, gains, cosine, sine):
    head_bits, outer_bits, ranks, heads, group = plan
    parts = 2 ** len(head_bits)
    relatives = 2 ** len(outer_bits)
    length = cosine.shape[0]
    model = weight_full.shape[0]
    rows = model // (parts * relatives)
    tokens = raw.shape[0]
    narrow, wide = context.shape[1], raw.shape[1]
    block_count = (relatives - 1) * parts + parts - 1
    half, width = length // 2, min(256, model)
    near = max(parts // 2, 1) * length
    anywhere = pl.BlockSpec(memory_space=pl.ANY)
    inside = pl.BlockSpec(memory_space=pltpu.VMEM)
    staged = max((relatives - 1) * parts, 1)
    spare = max(parts - 1, 1)
    many = parts > 1
    return pl.pallas_call(
        partial(scatter_kernel, plan),
        in_specs=[anywhere] * 4 + [inside] * 6,
        out_specs=[inside] * 4,
        out_shape=[
            jax.ShapeDtypeStruct((rows, parts * narrow), F32),
            jax.ShapeDtypeStruct((rows, parts * wide), F32),
            jax.ShapeDtypeStruct((length, model), BF16),
            jax.ShapeDtypeStruct((2, HEAD_SIZE), F32),
        ],
        scratch_shapes=[
            pltpu.VMEM((tokens, wide), BF16),
            pltpu.VMEM((near, wide) if many else (16, 128), BF16),
            pltpu.VMEM((2, tokens, rows), BF16),
            pltpu.VMEM((2, 2, width, wide), BF16),
            pltpu.VMEM((staged, rows, narrow), BF16),
            pltpu.VMEM((staged, rows, narrow), BF16),
            pltpu.VMEM((staged, rows, wide), BF16),
            pltpu.VMEM((staged, rows, wide), BF16),
            pltpu.VMEM((parts, rows, narrow), BF16),
            pltpu.VMEM((spare, rows, narrow), BF16),
            pltpu.VMEM((parts, rows, wide), BF16),
            pltpu.VMEM((spare, rows, wide), BF16),
            pltpu.VMEM((near, width) if many else (16, 128), F32),
            pltpu.VMEM((2, half, model) if many else (2, 16, 128), BF16),
            pltpu.VMEM((3, half, model) if many else (3, 16, 128), BF16),
            pltpu.VMEM((half, model) if many else (16, 128), BF16),
            pltpu.VMEM((half, model) if many else (16, 128), BF16),
            pltpu.SemaphoreType.DMA((2 * block_count + 8,)),
            pltpu.SemaphoreType.DMA((2 * block_count + 8,)),
            pltpu.SemaphoreType.DMA((2,)),
            pltpu.SemaphoreType.DMA((2, 2)),
        ],
        compiler_params=pltpu.CompilerParams(
            collective_id=1, has_side_effects=True, vmem_limit_bytes=63 * 1024 * 1024
        ),
        cost_estimate=pl.CostEstimate(
            flops=10**11, bytes_accessed=64 * length * model, transcendentals=length
        ),
        name="scatter_all",
    )(upstream_all, normed_all, weight_full, weight_other, context, context_grad, raw, gains, cosine, sine)


def local(hidden_in, upstream, merged_input_weight, output_matrix, norm_gain, query_gain, key_gain):
    shard_ranks = lax.axis_size("tensor")
    groups = lax.axis_size("dp")
    device = lax.axis_index("dp")
    query_heads = QUERY_HEADS // shard_ranks
    key_heads = KEY_VALUE_HEADS // shard_ranks
    group_width = QUERY_HEADS // KEY_VALUE_HEADS
    length, model = hidden_in.shape
    grad_scale = 1.0 / math.sqrt(groups * length)
    bits = device_bits(groups)
    head_bits = [1, 4] if key_heads % 4 == 0 and groups >= 8 and shard_ranks == 2 else []
    outer_bits = [bit for bit in bits if bit > 2 and bit not in head_bits]
    outer_bits += [bit for bit in bits if bit <= 2 and bit not in head_bits]
    parts = 2 ** len(head_bits)
    places = jnp.stack(block_places(head_bits, outer_bits, device)).astype(jnp.int32)
    part_queries = query_heads // parts
    part_keys = key_heads // parts
    query_columns = part_queries * HEAD_SIZE
    key_columns = part_keys * HEAD_SIZE
    plane = lax.axis_index("tensor")

    normed_all, upstream_all, weight_full, matrix_full, weight_other = gather_all(
        (head_bits, outer_bits, shard_ranks),
        hidden_in,
        upstream,
        merged_input_weight,
        output_matrix,
        norm_gain,
    )
    projected = jnp.dot(normed_all, weight_full, preferred_element_type=F32)
    cosine, sine = rope_tables(length, HEAD_SIZE)
    gains = jnp.stack([query_gain, key_gain])
    context_low = attention_forward(projected, gains, cosine, sine, part_keys, group_width)
    context_gradient = jnp.dot(
        upstream_all, matrix_full, preferred_element_type=F32
    ).astype(BF16)
    output_grad, input_grad, total_normed, head_sums = scatter_all(
        (head_bits, outer_bits, shard_ranks, part_keys, group_width),
        upstream_all,
        normed_all,
        weight_full,
        weight_other,
        context_low,
        context_gradient,
        projected,
        gains,
        cosine,
        sine,
    )
    shares = [total_normed]
    if parts == 1:
        for shift in range(1, shard_ranks):
            pairs = [(i, (i + shift) % shard_ranks) for i in range(shard_ranks)]
            shares.append(lax.ppermute(total_normed, "tensor", pairs))
    hidden_grad, gain_part = leave(places, hidden_in, upstream, norm_gain, shares)
    sums = jnp.concatenate([gain_part * (1.0 / shard_ranks), head_sums[0], head_sums[1]])
    sums = sum_all(sum_all(sums, "tensor"), "dp")
    gain_sum, query_sum, key_sum = jnp.split(sums, [model, model + HEAD_SIZE])
    return (
        hidden_grad,
        input_grad,
        output_grad,
        gain_sum * grad_scale,
        query_sum * grad_scale,
        key_sum * grad_scale,
    )


def solution(mesh):
    in_specs = (P("dp", None), P("dp", None), P("dp", "tensor"), P("dp", "tensor"), P(), P(), P())
    out_specs = (P("dp", None), P("dp", "tensor"), P("dp", "tensor"), P(), P(), P())
    return jax.shard_map(local, mesh=mesh, in_specs=in_specs, out_specs=out_specs, check_vma=False)
```

```python
from functools import partial
import math

import jax
import jax.numpy as jnp
import numpy as np
from jax import lax
from jax.experimental import pallas as pl
from jax.experimental.pallas import tpu as pltpu
from jax.sharding import PartitionSpec as P

QUERY_HEADS = 32
KEY_VALUE_HEADS = 8
HEAD_SIZE = 128


EPSILON = 1e-06
ROPE_BASE = 1000000.0
F32 = jnp.float32
BF16 = jnp.bfloat16
ROW_BLOCK = 128
MESH = pl.DeviceIdType.MESH


def rope_tables(length, columns):
    half_width = columns // 2
    exponent = np.arange(half_width, dtype=np.float32) * np.float32(2.0 / columns)
    frequency = np.exp(-exponent * np.float32(math.log(ROPE_BASE)))
    places = np.arange(length, dtype=np.float32)
    angles = places[:, None] * frequency[None, :]
    cosine, sine = np.cos(angles), np.sin(angles)
    return (
        jnp.asarray(np.concatenate([cosine, cosine], axis=1)),
        jnp.asarray(np.concatenate([-sine, sine], axis=1)),
    )


def call_params(vmem_mib):
    return pltpu.CompilerParams(
        dimension_semantics=("arbitrary",), vmem_limit_bytes=vmem_mib * 1024 * 1024
    )


def leave_kernel(places_ref, hidden_ref, upstream_ref, gain_ref, *rest):
    *shares, grad_ref, gain_grad_ref, natural = rest
    count = places_ref.shape[0]
    width = hidden_ref.shape[1] // count
    for at in range(count):
        target = pl.ds(pl.multiple_of(places_ref[at] * width, width), width)
        source = slice(at * width, (at + 1) * width)
        total = shares[0][:, source].astype(F32)
        for other in shares[1:]:
            total = total + other[:, source].astype(F32)
        natural[:, target] = total
    states = hidden_ref[...].astype(F32)
    inverse = lax.rsqrt(jnp.mean(states * states, axis=-1, keepdims=True) + EPSILON)
    unit = states * inverse
    part = jnp.sum(natural[...] * unit, axis=0, keepdims=True)

    @pl.when(pl.program_id(0) == 0)
    def _():
        gain_grad_ref[...] = part

    @pl.when(pl.program_id(0) != 0)
    def _():
        gain_grad_ref[...] += part

    scaled = natural[...] * gain_ref[...]
    mean = jnp.mean(scaled * unit, axis=-1, keepdims=True)
    grad = inverse * (scaled - unit * mean)
    grad_ref[...] = (upstream_ref[...].astype(F32) + grad).astype(BF16)


def leave(places, hidden_in, upstream, norm_gain, shares):
    length, model = hidden_in.shape
    block = min(length, ROW_BLOCK)
    whole = pl.BlockSpec((block, model), lambda i, places: (i, 0))
    line = pl.BlockSpec((1, model), lambda i, places: (0, 0))
    hidden_grad, gain_part = pl.pallas_call(
        leave_kernel,
        grid_spec=pltpu.PrefetchScalarGridSpec(
            num_scalar_prefetch=1,
            grid=(length // block,),
            in_specs=[whole, whole, line] + [whole] * len(shares),
            out_specs=[whole, line],
            scratch_shapes=[pltpu.VMEM((block, model), F32)],
        ),
        out_shape=[
            jax.ShapeDtypeStruct((length, model), BF16),
            jax.ShapeDtypeStruct((1, model), F32),
        ],
        compiler_params=call_params(40),
        cost_estimate=pl.CostEstimate(
            flops=12 * length * model,
            bytes_accessed=(6 + 2 * len(shares)) * length * model,
            transcendentals=length,
        ),
        name="leave",
    )(places, hidden_in, upstream, norm_gain.reshape(1, model), *shares)
    return hidden_grad, gain_part[0]


def turn(values):
    return pltpu.roll(values, HEAD_SIZE // 2, 1)


def head_states(raw, gain, cosine, sine):
    inverse = lax.rsqrt(jnp.mean(raw * raw, axis=-1, keepdims=True) + EPSILON)
    normed = raw * inverse * gain
    return (normed * cosine + turn(normed) * sine).astype(BF16)


def head_back(grad, raw, gain, cosine, sine):
    inverse = lax.rsqrt(jnp.mean(raw * raw, axis=-1, keepdims=True) + EPSILON)
    unit = raw * inverse
    grad_normed = grad * cosine + turn(grad * sine)
    part = jnp.sum(grad_normed * unit, axis=0, keepdims=True)
    scaled = grad_normed * gain
    mean = jnp.mean(scaled * unit, axis=-1, keepdims=True)
    return inverse * (scaled - unit * mean), part


def columns_of(index):
    return slice(index * HEAD_SIZE, (index + 1) * HEAD_SIZE)


def matmul(left, right, contract):
    return lax.dot_general(left, right, ((contract[:1], contract[1:]), ((), ())), preferred_element_type=F32)


def block_probs(queries, keys, tile, width, scale):
    scores = matmul(queries, keys, (1, 1)) * scale
    height = scores.shape[0]
    at_row = lax.rem(lax.broadcasted_iota(jnp.int32, (height, width), 0), tile) + (width - tile)
    causal = at_row >= lax.broadcasted_iota(jnp.int32, (height, width), 1)
    raised = jnp.where(causal, jnp.exp(scores), 0.0)
    return raised / jnp.sum(raised, axis=-1, keepdims=True)


def forward_kernel(heads, group, tile, raw_ref, gains_ref, cosine_ref, sine_ref, context_ref):
    length = raw_ref.shape[0]
    query_total = heads * group
    scale = 1.0 / math.sqrt(HEAD_SIZE)
    for head in range(heads):
        keys = head_states(
            raw_ref[:, columns_of(query_total + head)], gains_ref[1][...], cosine_ref[...], sine_ref[...]
        )
        values = raw_ref[:, columns_of(query_total + heads + head)].astype(BF16)
        for start in range(0, length, tile):
            rows = slice(start, start + tile)
            width = start + tile
            queries = jnp.concatenate(
                [
                    head_states(
                        raw_ref[rows, columns_of(head * group + one)],
                        gains_ref[0][...],
                        cosine_ref[rows],
                        sine_ref[rows],
                    )
                    for one in range(group)
                ],
                axis=0,
            )
            probs = block_probs(queries, keys[:width], tile, width, scale)
            context = matmul(probs.astype(BF16), values[:width], (1, 0)).astype(BF16)
            for one in range(group):
                context_ref[rows, columns_of(head * group + one)] = context[one * tile : (one + 1) * tile]


def backward_kernel(
    heads, group, tile, raw_ref, grad_ref, gains_ref, cosine_ref, sine_ref, out_ref, sums_ref, step
):
    length = raw_ref.shape[0]
    query_total = heads * group
    scale = 1.0 / math.sqrt(HEAD_SIZE)
    query_sum = jnp.zeros((1, HEAD_SIZE), F32)
    key_sum = jnp.zeros((1, HEAD_SIZE), F32)
    for head in range(heads):
        raw_keys = raw_ref[:, columns_of(query_total + head)]
        keys = head_states(raw_keys, gains_ref[1][...], cosine_ref[...], sine_ref[...])
        values = raw_ref[:, columns_of(query_total + heads + head)].astype(BF16)
        grad_keys = [jnp.zeros((tile, HEAD_SIZE), F32) for _ in range(length // tile)]
        grad_values = [jnp.zeros((tile, HEAD_SIZE), F32) for _ in range(length // tile)]
        for start in range(0, length, tile):
            rows = slice(start, start + tile)
            width = start + tile
            raw = jnp.concatenate(
                [raw_ref[rows, columns_of(head * group + one)] for one in range(group)], axis=0
            )
            cosine = jnp.concatenate([cosine_ref[rows]] * group, axis=0)
            sine = jnp.concatenate([sine_ref[rows]] * group, axis=0)
            queries = head_states(raw, gains_ref[0][...], cosine, sine)
            probs = block_probs(queries, keys[:width], tile, width, scale)
            probs_low = probs.astype(BF16)
            context_grad = jnp.concatenate(
                [grad_ref[rows, columns_of(head * group + one)] for one in range(group)], axis=0
            )
            grad_probs = matmul(context_grad, values[:width], (1, 1))
            centre = jnp.sum(probs * grad_probs, axis=-1, keepdims=True)
            grad_scores = (probs * (grad_probs - centre) * scale).astype(BF16)
            part_values = matmul(probs_low, context_grad, (0, 0))
            part_keys = matmul(grad_scores, queries, (0, 0))
            for at in range(width // tile):
                piece = slice(at * tile, (at + 1) * tile)
                grad_values[at] = grad_values[at] + part_values[piece]
                grad_keys[at] = grad_keys[at] + part_keys[piece]
            grad_queries = matmul(grad_scores, keys[:width], (1, 0))
            grad_raw, part = head_back(grad_queries, raw, gains_ref[0][...], cosine, sine)
            query_sum = query_sum + part
            grad_raw = grad_raw.astype(BF16)
            for one in range(group):
                out_ref[rows, columns_of(head * group + one)] = grad_raw[one * tile : (one + 1) * tile]
        grad_raw, part = head_back(
            jnp.concatenate(grad_keys, axis=0), raw_keys, gains_ref[1][...], cosine_ref[...], sine_ref[...]
        )
        key_sum = key_sum + part
        out_ref[:, columns_of(query_total + head)] = grad_raw.astype(BF16)
        out_ref[:, columns_of(query_total + heads + head)] = jnp.concatenate(
            grad_values, axis=0
        ).astype(BF16)
    sums = jnp.concatenate([query_sum, key_sum], axis=0)

    @pl.when(step == 0)
    def _():
        sums_ref[...] = sums

    @pl.when(step != 0)
    def _():
        sums_ref[...] += sums


def device_bits(count):
    bits = []
    bit = 1
    while bit < count:
        bits.append(bit)
        bit *= 2
    return bits


def bit_of(index, bit):
    return (index // bit) % 2


def sum_all(values, axis):
    count = lax.axis_size(axis)
    if count & (count - 1):
        return lax.psum(values, axis)
    step = 1
    while step < count:
        values = values + lax.ppermute(values, axis, [(i, i ^ step) for i in range(count)])
        step *= 2
    return values


def block_places(bits_inner, bits_outer, device):
    places = [(0, 0)]
    for bit in reversed(bits_inner):
        places = places + [(fixed | bit, relative) for fixed, relative in places]
    for bit in bits_outer:
        places = places + [(fixed, relative | bit) for fixed, relative in places]
    mask = sum(bits_outer)
    return [fixed + jnp.bitwise_xor(relative, jnp.bitwise_and(device, mask)) for fixed, relative in places]


def flipped(device, mask, bits):
    for bit in bits:
        if mask & bit:
            device = device + bit - 2 * bit * bit_of(device, bit)
    return device


def index_of(device, bits):
    return sum((bit_of(device, bit) * 2**at for at, bit in enumerate(bits)), 0 * device)


def masks_of(bits):
    masks = [0]
    for bit in bits:
        masks = masks + [mask | bit for mask in masks]
    return masks


class Copies:
    def __init__(self, send_sems, recv_sems):
        self.send_sems, self.recv_sems = send_sems, recv_sems
        self.names = {}
        self.started = []

    def place(self, name):
        return self.names.setdefault(name, len(self.names))

    def start(self, name, pairs, target):
        at = self.place(name)
        for source, destination in pairs:
            copy = pltpu.make_async_remote_copy(
                src_ref=source,
                dst_ref=destination,
                send_sem=self.send_sems.at[at],
                recv_sem=self.recv_sems.at[at],
                device_id=target,
                device_id_type=MESH,
            )
            copy.start()
        self.started.append(at)

    def wait(self, name, whole):
        at = self.place(name)
        pltpu.make_async_copy(whole, whole, self.recv_sems.at[at]).wait()

    def drain(self, name, whole):
        at = self.place(name)
        pltpu.make_async_copy(whole, whole, self.send_sems.at[at]).wait()


def gather_kernel(
    plan,
    hidden_ref,
    upstream_ref,
    weight_ref,
    matrix_ref,
    gain_ref,
    query_gain_ref,
    key_gain_ref,
    cosine_ref,
    sine_ref,
    normed_all,
    upstream_all,
    weight_full,
    matrix_full,
    weight_other,
    raw_ref,
    context_ref,
    context_grad_ref,
    normed_held,
    upstream_held,
    weight_near,
    matrix_near,
    tokens_near,
    context_sum,
    send_sems,
    recv_sems,
    local_sems,
    near_sems,
):
    head_bits, outer_bits, ranks, heads, cluster = plan
    gains_ref = (query_gain_ref, key_gain_ref)
    device = lax.axis_index("dp")
    plane = lax.axis_index("tensor")
    length, model = hidden_ref.shape
    rows = weight_ref.shape[0]
    parts = 2 ** len(head_bits)
    bits = head_bits + outer_bits
    slot_bits = head_bits[::-1]
    group = masks_of(head_bits)
    copies = Copies(send_sems, recv_sems)
    shared = ranks == 2 and any(bit > 1 for bit in head_bits)

    targets = [{"dp": flipped(device, mask, bits)} for mask in group[1:] + outer_bits]
    if shared:
        targets.append({"tensor": 1 - plane})
    barrier = pltpu.get_barrier_semaphore()
    for target in targets:
        pl.semaphore_signal(barrier, inc=1, device_id=target, device_id_type=MESH)
    pl.semaphore_wait(barrier, len(targets))

    def segments(full, ref):
        if full is weight_full:
            keys = KEY_VALUE_HEADS // ranks * HEAD_SIZE
            queries = QUERY_HEADS // ranks * HEAD_SIZE
            return [
                (0, queries // parts, 0),
                (queries, keys // parts, queries // parts),
                (queries + keys, keys // parts, (queries + keys) // parts),
            ]
        return [(0, ref.shape[1] // parts, 0)]

    def own_pairs(full, ref, mask):
        part = index_of(flipped(device, mask, bits), head_bits)
        first = pl.multiple_of(index_of(device, slot_bits) * rows, rows)
        pairs = []
        for start, width, place in segments(full, ref):
            source = ref.at[:, pl.ds(pl.multiple_of(start + part * width, HEAD_SIZE), width)]
            pairs.append((source, full.at[pl.ds(first, rows), pl.ds(place, width)]))
        return pairs

    def item(full, relative, mask):
        slot = index_of(flipped(device, mask, bits), slot_bits)
        first = pl.multiple_of((relative * parts + slot) * rows, rows)
        return full.at[pl.ds(first, rows), :]

    def base_start(name, full, ref):
        for mask in group[:0:-1]:
            copies.start((name, 0, mask), own_pairs(full, ref, mask), {"dp": flipped(device, mask, bits)})

    def outer_start(name, full, relative, mask, first_stage):
        for stage in range(first_stage, len(outer_bits)):
            bit = outer_bits[stage]
            landed = relative + 2**stage
            copies.start(
                (name, landed, mask),
                [(item(full, relative, mask), item(full, landed, mask))],
                {"dp": flipped(device, bit, bits)},
            )
        if full is weight_full and parts > 1:
            copies.start(
                ("x", relative, mask),
                [(item(full, relative, mask), item(weight_other, relative, mask))],
                {"dp": flipped(device, 1, bits)},
            )

    def arrive(name, full, relative, mask):
        copies.wait((name, relative, mask), item(full, relative, mask))
        stage = relative.bit_length()
        outer_start(name, full, relative, mask, stage)

    def place_own(full, ref, sem):
        pairs = own_pairs(full, ref, 0)
        for source, destination in pairs:
            pltpu.make_async_copy(source, destination, sem).start()

    def own_done(full, sem):
        whole = item(full, 0, 0)
        pltpu.make_async_copy(whole, whole, sem).wait()

    def sequence(full, index):
        return full.at[pl.ds(index * length, length), :]

    pieces = 2 if shared else 1
    height = length // (2 * pieces) if shared else length

    def piece_of(full, index, which, at):
        first = pl.multiple_of(index * length + (which * pieces + at) * height, height)
        return full.at[pl.ds(first, height), :]

    token_bits = head_bits[::-1]
    far = [bit for bit in token_bits if bit != 1]
    near = 2 ** len(far) if 1 in token_bits else 0

    here, there = (plane, 1 - plane) if shared else (0, 0)
    sibling = {"dp": flipped(device, 1, bits)}

    def tokens_start(name, full):
        if far:
            target = {"dp": flipped(device, far[0], bits)}
            for at in range(pieces):
                pair = (piece_of(full, 0, here, at), piece_of(full, 1, here, at))
                copies.start((name, "far", at), [pair], target)
        if near:
            copies.start((name, "near"), [(sequence(full, 0), sequence(full, near))], sibling)

    def tokens_far(name, full, at):
        if not far:
            return
        piece = piece_of(full, 1, here, at)
        copies.wait((name, "far", at), piece)
        if shared:
            copies.start((name, "side", at), [(piece, piece)], {"tensor": 1 - plane})
        if near:
            copies.start((name, "cross", at), [(piece, piece_of(full, near + 1, here, at))], sibling)

    def tokens_side(name, full, at):
        if not (far and shared):
            return
        piece = piece_of(full, 1, there, at)
        copies.wait((name, "side", at), piece)
        if near:
            copies.start((name, "over", at), [(piece, piece_of(full, near + 1, there, at))], sibling)

    def tokens_end(name, full):
        if near:
            copies.wait((name, "near"), sequence(full, near))
            for at in range(pieces if far else 0):
                copies.wait((name, "cross", at), piece_of(full, near + 1, here, at))
                if shared:
                    copies.wait((name, "over", at), piece_of(full, near + 1, there, at))

    relatives = list(range(1, 2 ** len(outer_bits)))
    last = 2 ** (len(outer_bits) - 1)
    early = [relative for relative in relatives if relative < last]
    late = [relative for relative in relatives if relative >= last]

    base_start("w", weight_full, weight_ref)
    place_own(weight_full, weight_ref, local_sems.at[0])
    own_done(weight_full, local_sems.at[0])

    inverse = lax.rsqrt(
        jnp.mean(jnp.square(hidden_ref[...].astype(F32)), axis=-1, keepdims=True) + EPSILON
    )
    for relative in range(2 ** len(outer_bits)):
        for slot in range(parts):
            owner = 0 * device
            for at, bit in enumerate(slot_bits):
                owner = owner + bit * ((slot >> at) & 1)
            for at, bit in enumerate(outer_bits):
                flag = bit_of(device, bit)
                owner = owner + bit * (flag + ((relative >> at) & 1) * (1 - 2 * flag))
            source = pl.ds(pl.multiple_of(owner * rows, rows), rows)
            target = pl.ds((relative * parts + slot) * rows, rows)
            piece = hidden_ref[:, source].astype(F32) * inverse * gain_ref[:, source]
            normed_held[:, target] = piece.astype(BF16)
            upstream_held[:, target] = upstream_ref[:, source]
    held_normed = pltpu.make_async_copy(normed_held, sequence(normed_all, 0), local_sems.at[1])
    held_normed.start()
    held_upstream = pltpu.make_async_copy(upstream_held, sequence(upstream_all, 0), local_sems.at[2])
    held_upstream.start()
    held_normed.wait()
    tokens_start("n", normed_all)
    outer_start("w", weight_full, 0, 0, 0)
    for mask in group[1:]:
        arrive("w", weight_full, 0, mask)
    held_upstream.wait()
    tokens_start("u", upstream_all)
    base_start("m", matrix_full, matrix_ref)
    place_own(matrix_full, matrix_ref, local_sems.at[3])
    own_done(matrix_full, local_sems.at[3])
    for at in range(pieces):
        tokens_far("n", normed_all, at)
    waiting = [(relative, mask) for relative in early for mask in group]
    for relative, mask in waiting[: len(waiting) // 2]:
        arrive("w", weight_full, relative, mask)
    for at in range(pieces):
        tokens_side("n", normed_all, at)
    for relative, mask in waiting[len(waiting) // 2 :]:
        arrive("w", weight_full, relative, mask)
    outer_start("m", matrix_full, 0, 0, 0)
    for relative in late:
        for mask in group:
            arrive("w", weight_full, relative, mask)
    load_weight = pltpu.make_async_copy(weight_full, weight_near, local_sems.at[4])
    load_weight.start()
    tokens_end("n", normed_all)

    def token_copy(full, index, columns):
        slot = lax.rem(index, 2)
        rows_of = pl.ds(pl.multiple_of(index * length, length), length)
        return pltpu.make_async_copy(
            full.at[rows_of, columns], tokens_near.at[slot, :, columns], near_sems.at[slot]
        )

    everything = pl.ds(0, model)
    token_copy(normed_all, 0, everything).start()
    load_weight.wait()

    def forward_step(index, carry):
        @pl.when(index + 1 < parts)
        def _():
            token_copy(normed_all, index + 1, everything).start()

        token_copy(normed_all, index, everything).wait()
        span = pl.ds(pl.multiple_of(index * length, length), length)
        raw_ref[span, :] = matmul(tokens_near[lax.rem(index, 2)], weight_near[...], (1, 0))
        forward_kernel(
            heads,
            cluster,
            min(length, ROW_BLOCK),
            raw_ref.at[span],
            gains_ref,
            cosine_ref,
            sine_ref,
            context_ref.at[span],
        )

        for at in range(pieces):

            @pl.when(index == max(parts - 3 + at, 0))
            def _(at=at):
                tokens_far("u", upstream_all, at)

        return carry

    lax.fori_loop(0, parts, forward_step, 0)
    for mask in group[1:]:
        arrive("m", matrix_full, 0, mask)
    for at in range(pieces):
        tokens_side("u", upstream_all, at)
    for relative in early:
        for mask in group:
            arrive("m", matrix_full, relative, mask)

    def context_half(which):
        columns = pl.ds(which * (model // 2), model // 2)
        load = pltpu.make_async_copy(
            matrix_full.at[columns, :], matrix_near.at[columns, :], local_sems.at[5 + which]
        )
        load.start()
        token_copy(upstream_all, 0, columns).start()
        load.wait()

        def step(index, carry):
            @pl.when(index + 1 < parts)
            def _():
                token_copy(upstream_all, index + 1, columns).start()

            token_copy(upstream_all, index, columns).wait()
            span = pl.ds(pl.multiple_of(index * length, length), length)
            part = matmul(tokens_near[lax.rem(index, 2), :, columns], matrix_near[columns, :], (1, 0))
            if which == 0:
                context_sum[span, :] = part
            else:
                context_grad_ref[span, :] = (context_sum[span, :] + part).astype(BF16)
            return carry

        lax.fori_loop(0, parts, step, 0)

    tokens_end("u", upstream_all)
    context_half(0)
    for relative in late:
        for mask in group:
            arrive("m", matrix_full, relative, mask)
    context_half(1)
    if parts > 1:
        for relative in range(2 ** len(outer_bits)):
            for mask in group:
                copies.wait(("x", relative, mask), item(weight_other, relative, mask))
                copies.drain(("x", relative, mask), item(weight_other, relative, mask))

    for name, full in (("w", weight_full), ("m", matrix_full)):
        for relative in range(2 ** len(outer_bits)):
            for mask in group:
                if relative or mask:
                    copies.drain((name, relative, mask), item(full, 0, 0))
    for name, full in (("n", normed_all), ("u", upstream_all)):
        for at in range(pieces if far else 0):
            piece = piece_of(full, 0, 0, 0)
            copies.drain((name, "far", at), piece)
            if shared:
                copies.drain((name, "side", at), piece)
            if near:
                copies.drain((name, "cross", at), piece)
                if shared:
                    copies.drain((name, "over", at), piece)
        if near:
            copies.drain((name, "near"), sequence(full, 0))


def gather_all(plan, hidden_in, upstream, weight, matrix, norm_gain, gains, cosine, sine):
    head_bits, outer_bits = plan[:2]
    length, model = hidden_in.shape
    parts = 2 ** len(head_bits)
    wide, narrow = weight.shape[1] // parts, matrix.shape[1] // parts
    count = 3 * (2 ** (len(outer_bits) + len(head_bits))) + 24
    anywhere = pl.BlockSpec(memory_space=pl.ANY)
    inside = pl.BlockSpec(memory_space=pltpu.VMEM)
    return pl.pallas_call(
        partial(gather_kernel, plan),
        in_specs=[inside] * 9,
        out_specs=[anywhere] * 5 + [inside] * 3,
        out_shape=[
            jax.ShapeDtypeStruct((parts * length, model), BF16),
            jax.ShapeDtypeStruct((parts * length, model), BF16),
            jax.ShapeDtypeStruct((model, weight.shape[1] // parts), BF16),
            jax.ShapeDtypeStruct((model, matrix.shape[1] // parts), BF16),
            jax.ShapeDtypeStruct((model if parts > 1 else 16, wide), BF16),
            jax.ShapeDtypeStruct((parts * length, wide), F32),
            jax.ShapeDtypeStruct((parts * length, narrow), BF16),
            jax.ShapeDtypeStruct((parts * length, narrow), BF16),
        ],
        scratch_shapes=[
            pltpu.VMEM((length, model), BF16),
            pltpu.VMEM((length, model), BF16),
            pltpu.VMEM((model, wide), BF16),
            pltpu.VMEM((model, narrow), BF16),
            pltpu.VMEM((2, length, model), BF16),
            pltpu.VMEM((parts * length, narrow), F32),
            pltpu.SemaphoreType.DMA((count,)),
            pltpu.SemaphoreType.DMA((count,)),
            pltpu.SemaphoreType.DMA((8,)),
            pltpu.SemaphoreType.DMA((2,)),
        ],
        compiler_params=pltpu.CompilerParams(
            collective_id=0, has_side_effects=True, vmem_limit_bytes=60 * 1024 * 1024
        ),
        cost_estimate=pl.CostEstimate(
            flops=10**11, bytes_accessed=64 * length * model, transcendentals=length
        ),
        name="gather_all",
    )(hidden_in, upstream, weight, matrix, norm_gain.reshape(1, model), *gains, cosine, sine)


def scatter_kernel(
    plan,
    upstream_all,
    normed_all,
    weight_full,
    weight_other,
    context_ref,
    context_grad_ref,
    raw_ref,
    query_gain_ref,
    key_gain_ref,
    cosine_ref,
    sine_ref,
    hidden_in,
    upstream_in,
    gain_ref,
    output_ref,
    input_ref,
    total_ref,
    sums_ref,
    gain_grad_ref,
    grad_ref,
    grad_other,
    left_held,
    weight_held,
    output_stage,
    output_landed,
    input_stage,
    input_landed,
    output_last,
    output_final,
    input_last,
    input_final,
    share_block,
    share_sent,
    share_got,
    share_own,
    share_far,
    send_sems,
    recv_sems,
    left_sems,
    weight_sems,
    leave_sems,
    gain_sent,
    gain_got,
):
    head_bits, outer_bits, ranks, heads, group = plan
    gains_ref = (query_gain_ref, key_gain_ref)
    device = lax.axis_index("dp")
    plane = lax.axis_index("tensor")
    parts = 2 ** len(head_bits)
    relatives = 2 ** len(outer_bits)
    length = cosine_ref.shape[0]
    model = weight_full.shape[0]
    rows = model // (parts * relatives)
    bits = head_bits + outer_bits
    slot_bits = head_bits[::-1]
    masks = masks_of(head_bits)
    scale = 1.0 / math.sqrt(lax.axis_size("dp") * length)
    copies = Copies(send_sems, recv_sems)

    outer_masks = masks_of(outer_bits)[1:] if parts > 1 else outer_bits
    targets = [{"dp": flipped(device, mask, bits)} for mask in masks[1:] + outer_masks]
    if parts > 1:
        targets.append({"tensor": 1 - plane})
    barrier = pltpu.get_barrier_semaphore()
    for target in targets:
        pl.semaphore_signal(barrier, inc=1, device_id=target, device_id_type=MESH)
    pl.semaphore_wait(barrier, len(targets))

    kinds = {
        "o": (upstream_all, context_ref, output_stage, output_landed, output_last, output_final, output_ref),
        "g": (normed_all, grad_ref, input_stage, input_landed, input_last, input_final, input_ref),
    }
    blocks = {"o": 0, "g": (relatives - 1) * parts + parts - 1}
    block_count = (relatives - 1) * parts + parts - 1

    def partner(mask_index):
        target, slot = device, 0 * device
        for at, bit in enumerate(head_bits):
            change = (mask_index // 2**at) % 2
            flag = bit_of(device, bit)
            target = target + bit * change * (1 - 2 * flag)
            slot = slot + 2 ** slot_bits.index(bit) * (flag + change - 2 * flag * change)
        return target, slot

    def left_copy(kind, relative, index):
        _, slot = partner(index)
        first = pl.multiple_of((relative * parts + slot) * rows, rows)
        return pltpu.make_async_copy(
            kinds[kind][0].at[:, pl.ds(first, rows)],
            left_held.at[lax.rem(index, 2)],
            left_sems.at[lax.rem(index, 2)],
        )

    def remote(kind, at, source, destination, target):
        return pltpu.make_async_remote_copy(
            src_ref=source,
            dst_ref=destination,
            send_sem=send_sems.at[blocks[kind] + at],
            recv_sem=recv_sems.at[blocks[kind] + at],
            device_id=target,
            device_id_type=MESH,
        )

    def handle(kind, relative, index):
        _, right, stage, landed, last, final, result = kinds[kind]

        @pl.when(index + 1 < parts)
        def _():
            left_copy(kind, relative, index + 1).start()

        left_copy(kind, relative, index).wait()
        total = matmul(left_held[lax.rem(index, 2)], right[...], (0, 0))
        top = relative.bit_length()
        for later in range(top, len(outer_bits)):
            source = relative + 2**later
            at = (source - 1) * parts + index
            piece = landed.at[at]
            pltpu.make_async_copy(piece, piece, recv_sems.at[blocks[kind] + at]).wait()
            total = total + piece[...].astype(F32)
        if relative:
            at = (relative - 1) * parts + index
            stage[at] = total.astype(BF16)
            target = {"dp": flipped(device, outer_bits[top - 1], bits)}
            remote(kind, at, stage.at[at], landed.at[at], target).start()
        else:
            last[index] = total.astype(BF16)

            @pl.when(index > 0)
            def _():
                target, _ = partner(index)
                at = (relatives - 1) * parts + index - 1
                remote(kind, at, last.at[index], final.at[index - 1], {"dp": target}).start()

    def process(kind, relative):
        left_copy(kind, relative, 0).start()

        def body(index, carry):
            handle(kind, relative, index)
            return carry

        lax.fori_loop(0, parts, body, 0)

    for relative in range(relatives - 1, 1, -1):
        process("o", relative)

    left_copy("o", 1, 0).start()

    def sequence_step(index, carry):
        span = pl.ds(pl.multiple_of(index * length, length), length)
        backward_kernel(
            heads,
            group,
            min(length, ROW_BLOCK),
            raw_ref.at[span],
            context_grad_ref.at[span],
            gains_ref,
            cosine_ref,
            sine_ref,
            grad_ref.at[span],
            sums_ref,
            index,
        )
        handle("o", 1, index)
        return carry

    lax.fori_loop(0, parts, sequence_step, 0)

    if parts > 1:
        near = (parts // 2) * length
        copies.names = {("skip", at): at for at in range(2 * block_count)}
        copies.start(
            "grad",
            [(grad_ref.at[pl.ds(near, near)], grad_other)],
            {"dp": flipped(device, 1, bits)},
        )

    width = weight_held.shape[2]
    weight_blocks = model // width

    def weight_copies(index):
        slot = lax.rem(index, 2)
        span = pl.ds(pl.multiple_of(index * width, width), width)
        pairs = [(weight_full, 0)] + ([(weight_other, 1)] if parts > 1 else [])
        return [
            pltpu.make_async_copy(full.at[span], weight_held.at[slot, at], weight_sems.at[slot, at])
            for full, at in pairs
        ]

    half = length // 2
    mine = pl.ds(pl.multiple_of(plane % 2 * half, half), half)
    theirs = pl.ds(pl.multiple_of((1 - plane % 2) * half, half), half)
    taken = (parts // 2) * length if parts > 1 else length

    for copy in weight_copies(0):
        copy.start()
    if parts > 1:
        copies.wait("grad", grad_other)

    side = {"tensor": 1 - plane}
    halves = [pl.ds(at * (model // 2), model // 2) for at in range(2)]

    def side_start(at):
        copies.start(
            ("side", at),
            [(share_sent.at[0, :, halves[at]], share_got.at[0, :, halves[at]])],
            side,
        )

    def weight_step(index, carry):
        @pl.when(index + 1 < weight_blocks)
        def _():
            for copy in weight_copies(index + 1):
                copy.start()

        for copy in weight_copies(index):
            copy.wait()
        slot = lax.rem(index, 2)
        span = pl.ds(pl.multiple_of(index * width, width), width)
        share = matmul(grad_ref[0:taken], weight_held[slot, 0], (1, 1))
        if parts > 1:
            share = share + matmul(grad_other[...], weight_held[slot, 1], (1, 1))
            share_block[...] = share
            far_mine = pl.ds(pl.multiple_of(length + plane % 2 * half, half), half)
            far_theirs = pl.ds(pl.multiple_of(length + (1 - plane % 2) * half, half), half)
            share_far[:, span] = share_block[far_mine, :].astype(BF16)
            share_sent[0, :, span] = share_block[far_theirs, :].astype(BF16)
            share_own[:, span] = share_block[mine, :].astype(BF16)
            share_sent[1, :, span] = share_block[theirs, :].astype(BF16)

            @pl.when(index == weight_blocks // 2 - 1)
            def _():
                side_start(0)

            @pl.when(index == weight_blocks - 1)
            def _():
                side_start(1)

        else:
            total_ref[:, span] = share.astype(BF16)
        return carry

    lax.fori_loop(0, weight_blocks, weight_step, 0)
    across = {"dp": flipped(device, 4, bits)}

    def across_start(at):
        where = halves[at]
        copies.wait(("side", at), share_got.at[0, :, where])
        share_far[:, where] = (
            share_far[:, where].astype(F32) + share_got[0, :, where].astype(F32)
        ).astype(BF16)
        copies.start(
            ("across", at), [(share_far.at[:, where], share_got.at[2, :, where])], across
        )

    def back_start(at):
        where = halves[at]
        copies.wait(("across", at), share_got.at[2, :, where])
        share_own[:, where] = (
            share_own[:, where].astype(F32)
            + share_got[1, :, where].astype(F32)
            + share_got[2, :, where].astype(F32)
        ).astype(BF16)
        total_ref[mine, where] = share_own[:, where]
        copies.start(
            ("back", at), [(share_own.at[:, where], total_ref.at[mine, where])], side
        )

    if parts > 1:
        copies.start("rest", [(share_sent.at[1], share_got.at[1])], side)
    for relative in range(relatives - 1, 1, -1):
        process("g", relative)
    if parts > 1:
        across_start(0)
    process("o", 0)
    if parts > 1:
        across_start(1)
    if relatives > 1:
        process("g", 1)
    if parts > 1:
        copies.wait("rest", share_got.at[1])
        back_start(0)
        back_start(1)
        copies.drain("rest", share_own)
        for name in ("side", "across"):
            for at in range(2):
                copies.drain((name, at), share_far.at[:, halves[at]])
        gain_grad_ref[...] = jnp.zeros_like(gain_grad_ref)
        loads = [
            pltpu.make_async_copy(full.at[where], buffer, leave_sems.at[at])
            for at, (full, where, buffer) in enumerate(
                [
                    (hidden_in, mine, share_sent.at[0]),
                    (upstream_in, mine, share_sent.at[1]),
                    (hidden_in, theirs, share_got.at[0]),
                    (upstream_in, theirs, share_got.at[1]),
                ]
            )
        ]
        for load in loads:
            load.start()
        for load in loads:
            load.wait()

    owners = []
    for relative in range(relatives):
        for slot in range(parts):
            owner = 0 * device
            for at, bit in enumerate(slot_bits):
                owner = owner + bit * ((slot >> at) & 1)
            for at, bit in enumerate(outer_bits):
                flag = bit_of(device, bit)
                owner = owner + bit * (flag + ((relative >> at) & 1) * (1 - 2 * flag))
            owners.append(owner)

    def leave_half(first_row, buffers):
        step_rows = 32

        def step(index, carry):
            there = pl.ds(pl.multiple_of(first_row + index * step_rows, step_rows), step_rows)
            span = pl.ds(pl.multiple_of(index * step_rows, step_rows), step_rows)
            for at, owner in enumerate(owners):
                share_far[span, pl.ds(pl.multiple_of(owner * rows, rows), rows)] = total_ref[
                    there, at * rows : (at + 1) * rows
                ]
            states = buffers[0][span, :].astype(F32)
            inverse = lax.rsqrt(jnp.mean(states * states, axis=-1, keepdims=True) + EPSILON)
            unit = states * inverse
            grad = share_far[span, :].astype(F32)
            gain_grad_ref[...] += jnp.sum(grad * unit, axis=0, keepdims=True)
            scaled = grad * gain_ref[...]
            mean = jnp.mean(scaled * unit, axis=-1, keepdims=True)
            result = buffers[1][span, :].astype(F32) + inverse * (scaled - unit * mean)
            total_ref[there, :] = result.astype(BF16)
            return carry

        lax.fori_loop(0, half // step_rows, step, 0)

    if parts > 1:
        leave_half(plane % 2 * half, (share_sent.at[0], share_sent.at[1]))
    process("g", 0)

    def finish(kind, indices):
        _, _, stage, _, last, final, result = kinds[kind]
        if kind == "o":
            spans = [(0, heads * group * HEAD_SIZE, 0)]
        else:
            query, key = heads * group * HEAD_SIZE, heads * HEAD_SIZE
            spans = [
                (0, query, 0),
                (query, key, parts * query),
                (query + key, key, parts * (query + key)),
            ]
        for index in indices:
            if index:
                at = (relatives - 1) * parts + index - 1
                piece = final.at[index - 1]
                pltpu.make_async_copy(piece, piece, recv_sems.at[blocks[kind] + at]).wait()
            values = (last[0] if index == 0 else final[index - 1]).astype(F32) * scale
            part = index_of(flipped(device, masks[index], bits), head_bits)
            for start, columns, place in spans:
                result[:, pl.ds(pl.multiple_of(place + part * columns, HEAD_SIZE), columns)] = values[
                    :, start : start + columns
                ]

    finish("o", range(parts))
    if parts > 1:
        for at in range(2):
            copies.wait(("back", at), total_ref.at[theirs, halves[at]])
        leave_half((1 - plane % 2) * half, (share_got.at[0], share_got.at[1]))
        gain_sent[0, :, :model] = gain_grad_ref[...] * (1.0 / ranks)
        gain_sent[0, :, model : model + HEAD_SIZE] = sums_ref[0:1]
        gain_sent[0, :, model + HEAD_SIZE :] = sums_ref[1:2]
        stages = [
            [{"dp": flipped(device, mask, bits)} for mask in masks[1:]],
            [{"dp": flipped(device, mask, bits)} for mask in outer_masks],
            [side],
        ]

        def gains_start(stage):
            for at, target in enumerate(stages[stage]):
                copies.start(
                    ("gain", stage, at),
                    [(gain_sent.at[stage], gain_got.at[3 * stage + at])],
                    target,
                )

        def gains_end(stage):
            terms = [gain_sent[stage]]
            for at in range(len(stages[stage])):
                place = gain_got.at[3 * stage + at]
                copies.wait(("gain", stage, at), place)
                terms.append(place[...])
            while len(terms) > 1:
                terms = [terms[at] + terms[at + 1] for at in range(0, len(terms), 2)]
            return terms[0]

        gains_start(0)
        finish("g", range(0, 2))
        gain_sent[1] = gains_end(0)
        gains_start(1)
        finish("g", range(2, parts))
        gain_sent[2] = gains_end(1)
        gains_start(2)
        gain_total = gains_end(2) * scale
        gain_grad_ref[...] = gain_total[:, :model]
        sums_ref[0:1] = gain_total[:, model : model + HEAD_SIZE]
        sums_ref[1:2] = gain_total[:, model + HEAD_SIZE :]
        for stage in range(3):
            for at in range(len(stages[stage])):
                copies.drain(("gain", stage, at), gain_sent.at[0])
    else:
        gain_grad_ref[...] = jnp.zeros_like(gain_grad_ref)
        finish("g", range(parts))

    for kind in ("o", "g"):
        _, _, stage, _, last, _, _ = kinds[kind]
        for at in range(block_count):
            piece = stage.at[0]
            pltpu.make_async_copy(piece, piece, send_sems.at[blocks[kind] + at]).wait()
    if parts > 1:
        copies.drain("grad", grad_other)
        for at in range(2):
            copies.drain(("back", at), share_far.at[:, halves[at]])


def scatter_all(plan, upstream_all, normed_all, weight_full, weight_other, *rest):
    context, _, raw, _, _, cosine = rest[:6]
    head_bits, outer_bits, ranks, heads, group = plan
    parts = 2 ** len(head_bits)
    relatives = 2 ** len(outer_bits)
    length = cosine.shape[0]
    model = weight_full.shape[0]
    rows = model // (parts * relatives)
    tokens = raw.shape[0]
    narrow, wide = context.shape[1], raw.shape[1]
    block_count = (relatives - 1) * parts + parts - 1
    half, width = length // 2, min(256, model)
    near = max(parts // 2, 1) * length
    anywhere = pl.BlockSpec(memory_space=pl.ANY)
    inside = pl.BlockSpec(memory_space=pltpu.VMEM)
    staged = max((relatives - 1) * parts, 1)
    spare = max(parts - 1, 1)
    many = parts > 1
    return pl.pallas_call(
        partial(scatter_kernel, plan),
        in_specs=[anywhere] * 4 + [inside] * 7 + [anywhere] * 2 + [inside],
        out_specs=[inside] * 5,
        out_shape=[
            jax.ShapeDtypeStruct((rows, parts * narrow), F32),
            jax.ShapeDtypeStruct((rows, parts * wide), F32),
            jax.ShapeDtypeStruct((length, model), BF16),
            jax.ShapeDtypeStruct((2, HEAD_SIZE), F32),
            jax.ShapeDtypeStruct((1, model), F32),
        ],
        scratch_shapes=[
            pltpu.VMEM((tokens, wide), BF16),
            pltpu.VMEM((near, wide) if many else (16, 128), BF16),
            pltpu.VMEM((2, tokens, rows), BF16),
            pltpu.VMEM((2, 2, width, wide), BF16),
            pltpu.VMEM((staged, rows, narrow), BF16),
            pltpu.VMEM((staged, rows, narrow), BF16),
            pltpu.VMEM((staged, rows, wide), BF16),
            pltpu.VMEM((staged, rows, wide), BF16),
            pltpu.VMEM((parts, rows, narrow), BF16),
            pltpu.VMEM((spare, rows, narrow), BF16),
            pltpu.VMEM((parts, rows, wide), BF16),
            pltpu.VMEM((spare, rows, wide), BF16),
            pltpu.VMEM((near, width) if many else (16, 128), F32),
            pltpu.VMEM((2, half, model) if many else (2, 16, 128), BF16),
            pltpu.VMEM((3, half, model) if many else (3, 16, 128), BF16),
            pltpu.VMEM((half, model) if many else (16, 128), BF16),
            pltpu.VMEM((half, model) if many else (16, 128), BF16),
            pltpu.SemaphoreType.DMA((2 * block_count + 16,)),
            pltpu.SemaphoreType.DMA((2 * block_count + 16,)),
            pltpu.SemaphoreType.DMA((2,)),
            pltpu.SemaphoreType.DMA((2, 2)),
            pltpu.SemaphoreType.DMA((4,)),
            pltpu.VMEM((3, 1, model + 2 * HEAD_SIZE), F32),
            pltpu.VMEM((7, 1, model + 2 * HEAD_SIZE), F32),
        ],
        compiler_params=pltpu.CompilerParams(
            collective_id=1, has_side_effects=True, vmem_limit_bytes=63 * 1024 * 1024
        ),
        cost_estimate=pl.CostEstimate(
            flops=10**11, bytes_accessed=64 * length * model, transcendentals=length
        ),
        name="scatter_all",
    )(upstream_all, normed_all, weight_full, weight_other, *rest)


def local(hidden_in, upstream, merged_input_weight, output_matrix, norm_gain, query_gain, key_gain):
    shard_ranks = lax.axis_size("tensor")
    groups = lax.axis_size("dp")
    device = lax.axis_index("dp")
    key_heads = KEY_VALUE_HEADS // shard_ranks
    group_width = QUERY_HEADS // KEY_VALUE_HEADS
    length, model = hidden_in.shape
    grad_scale = 1.0 / math.sqrt(groups * length)
    bits = device_bits(groups)
    head_bits = [1, 4] if key_heads % 4 == 0 and groups >= 8 and shard_ranks == 2 else []
    outer_bits = [bit for bit in bits if bit > 2 and bit not in head_bits]
    outer_bits += [bit for bit in bits if bit <= 2 and bit not in head_bits]
    parts = 2 ** len(head_bits)
    part_keys = key_heads // parts
    cosine, sine = rope_tables(length, HEAD_SIZE)
    gains = (query_gain.reshape(1, HEAD_SIZE), key_gain.reshape(1, HEAD_SIZE))
    plan = (head_bits, outer_bits, shard_ranks, part_keys, group_width)
    gathered = gather_all(
        plan,
        hidden_in,
        upstream,
        merged_input_weight,
        output_matrix,
        norm_gain,
        gains,
        cosine,
        sine,
    )
    normed_all, upstream_all, weight_full, _, weight_other = gathered[:5]
    projected, context_low, context_gradient = gathered[5:]
    output_grad, input_grad, hidden_grad, head_sums, gain_part = scatter_all(
        plan,
        upstream_all,
        normed_all,
        weight_full,
        weight_other,
        context_low,
        context_gradient,
        projected,
        *gains,
        cosine,
        sine,
        hidden_in,
        upstream,
        norm_gain.reshape(1, model),
    )
    if parts == 1:
        shares = [hidden_grad]
        for shift in range(1, shard_ranks):
            pairs = [(i, (i + shift) % shard_ranks) for i in range(shard_ranks)]
            shares.append(lax.ppermute(hidden_grad, "tensor", pairs))
        places = jnp.stack(block_places(head_bits, outer_bits, device)).astype(jnp.int32)
        hidden_grad, gain_part = leave(places, hidden_in, upstream, norm_gain, shares)
        sums = jnp.concatenate([gain_part * (1.0 / shard_ranks), head_sums[0], head_sums[1]])
        sums = sum_all(sum_all(sums, "tensor"), "dp") * grad_scale
        gain_grad, query_grad, key_grad = jnp.split(sums, [model, model + HEAD_SIZE])
    else:
        gain_grad, query_grad, key_grad = gain_part[0], head_sums[0], head_sums[1]
    return (
        hidden_grad,
        input_grad,
        output_grad,
        gain_grad,
        query_grad,
        key_grad,
    )


def solution(mesh):
    in_specs = (P("dp", None), P("dp", None), P("dp", "tensor"), P("dp", "tensor"), P(), P(), P())
    out_specs = (P("dp", None), P("dp", "tensor"), P("dp", "tensor"), P(), P(), P())
    return jax.shard_map(local, mesh=mesh, in_specs=in_specs, out_specs=out_specs, check_vma=False)
```

```python
from functools import partial
import math

import jax
import jax.numpy as jnp
import numpy as np
from jax import lax
from jax.experimental import pallas as pl
from jax.experimental.pallas import tpu as pltpu
from jax.sharding import PartitionSpec as P

QUERY_HEADS = 32
KEY_VALUE_HEADS = 8
HEAD_SIZE = 128


EPSILON = 1e-06
ROPE_BASE = 1000000.0
F32 = jnp.float32
BF16 = jnp.bfloat16
ROW_BLOCK = 128
MESH = pl.DeviceIdType.MESH


def rope_tables(length, columns):
    half_width = columns // 2
    exponent = np.arange(half_width, dtype=np.float32) * np.float32(2.0 / columns)
    frequency = np.exp(-exponent * np.float32(math.log(ROPE_BASE)))
    places = np.arange(length, dtype=np.float32)
    angles = places[:, None] * frequency[None, :]
    cosine, sine = np.cos(angles), np.sin(angles)
    return (
        jnp.asarray(np.concatenate([cosine, cosine], axis=1)),
        jnp.asarray(np.concatenate([-sine, sine], axis=1)),
    )


def call_params(vmem_mib):
    return pltpu.CompilerParams(
        dimension_semantics=("arbitrary",), vmem_limit_bytes=vmem_mib * 1024 * 1024
    )


def leave_kernel(places_ref, hidden_ref, upstream_ref, gain_ref, *rest):
    *shares, grad_ref, gain_grad_ref, natural = rest
    count = places_ref.shape[0]
    width = hidden_ref.shape[1] // count
    for at in range(count):
        target = pl.ds(pl.multiple_of(places_ref[at] * width, width), width)
        source = slice(at * width, (at + 1) * width)
        total = shares[0][:, source].astype(F32)
        for other in shares[1:]:
            total = total + other[:, source].astype(F32)
        natural[:, target] = total
    states = hidden_ref[...].astype(F32)
    inverse = lax.rsqrt(jnp.mean(states * states, axis=-1, keepdims=True) + EPSILON)
    unit = states * inverse
    part = jnp.sum(natural[...] * unit, axis=0, keepdims=True)

    @pl.when(pl.program_id(0) == 0)
    def _():
        gain_grad_ref[...] = part

    @pl.when(pl.program_id(0) != 0)
    def _():
        gain_grad_ref[...] += part

    scaled = natural[...] * gain_ref[...]
    mean = jnp.mean(scaled * unit, axis=-1, keepdims=True)
    grad = inverse * (scaled - unit * mean)
    grad_ref[...] = (upstream_ref[...].astype(F32) + grad).astype(BF16)


def leave(places, hidden_in, upstream, norm_gain, shares):
    length, model = hidden_in.shape
    block = min(length, ROW_BLOCK)
    whole = pl.BlockSpec((block, model), lambda i, places: (i, 0))
    line = pl.BlockSpec((1, model), lambda i, places: (0, 0))
    hidden_grad, gain_part = pl.pallas_call(
        leave_kernel,
        grid_spec=pltpu.PrefetchScalarGridSpec(
            num_scalar_prefetch=1,
            grid=(length // block,),
            in_specs=[whole, whole, line] + [whole] * len(shares),
            out_specs=[whole, line],
            scratch_shapes=[pltpu.VMEM((block, model), F32)],
        ),
        out_shape=[
            jax.ShapeDtypeStruct((length, model), BF16),
            jax.ShapeDtypeStruct((1, model), F32),
        ],
        compiler_params=call_params(40),
        cost_estimate=pl.CostEstimate(
            flops=12 * length * model,
            bytes_accessed=(6 + 2 * len(shares)) * length * model,
            transcendentals=length,
        ),
        name="leave",
    )(places, hidden_in, upstream, norm_gain.reshape(1, model), *shares)
    return hidden_grad, gain_part[0]


def turn(values):
    return pltpu.roll(values, HEAD_SIZE // 2, 1)


def head_states(raw, gain, cosine, sine):
    inverse = lax.rsqrt(jnp.mean(raw * raw, axis=-1, keepdims=True) + EPSILON)
    normed = raw * inverse * gain
    return (normed * cosine + turn(normed) * sine).astype(BF16)


def head_back(grad, raw, gain, cosine, sine):
    inverse = lax.rsqrt(jnp.mean(raw * raw, axis=-1, keepdims=True) + EPSILON)
    unit = raw * inverse
    grad_normed = grad * cosine + turn(grad * sine)
    part = jnp.sum(grad_normed * unit, axis=0, keepdims=True)
    scaled = grad_normed * gain
    mean = jnp.mean(scaled * unit, axis=-1, keepdims=True)
    return inverse * (scaled - unit * mean), part


def columns_of(index):
    return slice(index * HEAD_SIZE, (index + 1) * HEAD_SIZE)


def matmul(left, right, contract):
    return lax.dot_general(left, right, ((contract[:1], contract[1:]), ((), ())), preferred_element_type=F32)


def block_probs(queries, keys, tile, width, scale):
    scores = matmul(queries, keys, (1, 1)) * scale
    height = scores.shape[0]
    at_row = lax.rem(lax.broadcasted_iota(jnp.int32, (height, width), 0), tile) + (width - tile)
    causal = at_row >= lax.broadcasted_iota(jnp.int32, (height, width), 1)
    raised = jnp.where(causal, jnp.exp(scores), 0.0)
    return raised / jnp.sum(raised, axis=-1, keepdims=True)


def forward_kernel(heads, group, tile, raw_ref, gains_ref, cosine_ref, sine_ref, context_ref):
    length = raw_ref.shape[0]
    query_total = heads * group
    scale = 1.0 / math.sqrt(HEAD_SIZE)
    for head in range(heads):
        keys = head_states(
            raw_ref[:, columns_of(query_total + head)], gains_ref[1][...], cosine_ref[...], sine_ref[...]
        )
        values = raw_ref[:, columns_of(query_total + heads + head)].astype(BF16)
        for start in range(0, length, tile):
            rows = slice(start, start + tile)
            width = start + tile
            queries = jnp.concatenate(
                [
                    head_states(
                        raw_ref[rows, columns_of(head * group + one)],
                        gains_ref[0][...],
                        cosine_ref[rows],
                        sine_ref[rows],
                    )
                    for one in range(group)
                ],
                axis=0,
            )
            probs = block_probs(queries, keys[:width], tile, width, scale)
            context = matmul(probs.astype(BF16), values[:width], (1, 0)).astype(BF16)
            for one in range(group):
                context_ref[rows, columns_of(head * group + one)] = context[one * tile : (one + 1) * tile]


def backward_kernel(
    heads, group, tile, raw_ref, grad_ref, gains_ref, cosine_ref, sine_ref, out_ref, sums_ref, step
):
    length = raw_ref.shape[0]
    query_total = heads * group
    scale = 1.0 / math.sqrt(HEAD_SIZE)
    query_sum = jnp.zeros((1, HEAD_SIZE), F32)
    key_sum = jnp.zeros((1, HEAD_SIZE), F32)
    for head in range(heads):
        raw_keys = raw_ref[:, columns_of(query_total + head)]
        keys = head_states(raw_keys, gains_ref[1][...], cosine_ref[...], sine_ref[...])
        values = raw_ref[:, columns_of(query_total + heads + head)].astype(BF16)
        grad_keys = [jnp.zeros((tile, HEAD_SIZE), F32) for _ in range(length // tile)]
        grad_values = [jnp.zeros((tile, HEAD_SIZE), F32) for _ in range(length // tile)]
        for start in range(0, length, tile):
            rows = slice(start, start + tile)
            width = start + tile
            raw = jnp.concatenate(
                [raw_ref[rows, columns_of(head * group + one)] for one in range(group)], axis=0
            )
            cosine = jnp.concatenate([cosine_ref[rows]] * group, axis=0)
            sine = jnp.concatenate([sine_ref[rows]] * group, axis=0)
            queries = head_states(raw, gains_ref[0][...], cosine, sine)
            probs = block_probs(queries, keys[:width], tile, width, scale)
            probs_low = probs.astype(BF16)
            context_grad = jnp.concatenate(
                [grad_ref[rows, columns_of(head * group + one)] for one in range(group)], axis=0
            )
            grad_probs = matmul(context_grad, values[:width], (1, 1))
            centre = jnp.sum(probs * grad_probs, axis=-1, keepdims=True)
            grad_scores = (probs * (grad_probs - centre) * scale).astype(BF16)
            part_values = matmul(probs_low, context_grad, (0, 0))
            part_keys = matmul(grad_scores, queries, (0, 0))
            for at in range(width // tile):
                piece = slice(at * tile, (at + 1) * tile)
                grad_values[at] = grad_values[at] + part_values[piece]
                grad_keys[at] = grad_keys[at] + part_keys[piece]
            grad_queries = matmul(grad_scores, keys[:width], (1, 0))
            grad_raw, part = head_back(grad_queries, raw, gains_ref[0][...], cosine, sine)
            query_sum = query_sum + part
            grad_raw = grad_raw.astype(BF16)
            for one in range(group):
                out_ref[rows, columns_of(head * group + one)] = grad_raw[one * tile : (one + 1) * tile]
        grad_raw, part = head_back(
            jnp.concatenate(grad_keys, axis=0), raw_keys, gains_ref[1][...], cosine_ref[...], sine_ref[...]
        )
        key_sum = key_sum + part
        out_ref[:, columns_of(query_total + head)] = grad_raw.astype(BF16)
        out_ref[:, columns_of(query_total + heads + head)] = jnp.concatenate(
            grad_values, axis=0
        ).astype(BF16)
    sums = jnp.concatenate([query_sum, key_sum], axis=0)

    @pl.when(step == 0)
    def _():
        sums_ref[...] = sums

    @pl.when(step != 0)
    def _():
        sums_ref[...] += sums


def device_bits(count):
    bits = []
    bit = 1
    while bit < count:
        bits.append(bit)
        bit *= 2
    return bits


def bit_of(index, bit):
    return (index // bit) % 2


def sum_all(values, axis):
    count = lax.axis_size(axis)
    if count & (count - 1):
        return lax.psum(values, axis)
    step = 1
    while step < count:
        values = values + lax.ppermute(values, axis, [(i, i ^ step) for i in range(count)])
        step *= 2
    return values


def block_places(bits_inner, bits_outer, device):
    places = [(0, 0)]
    for bit in reversed(bits_inner):
        places = places + [(fixed | bit, relative) for fixed, relative in places]
    for bit in bits_outer:
        places = places + [(fixed, relative | bit) for fixed, relative in places]
    mask = sum(bits_outer)
    return [fixed + jnp.bitwise_xor(relative, jnp.bitwise_and(device, mask)) for fixed, relative in places]


def flipped(device, mask, bits):
    for bit in bits:
        if mask & bit:
            device = device + bit - 2 * bit * bit_of(device, bit)
    return device


def index_of(device, bits):
    return sum((bit_of(device, bit) * 2**at for at, bit in enumerate(bits)), 0 * device)


def masks_of(bits):
    masks = [0]
    for bit in bits:
        masks = masks + [mask | bit for mask in masks]
    return masks


class Copies:
    def __init__(self, send_sems, recv_sems):
        self.send_sems, self.recv_sems = send_sems, recv_sems
        self.names = {}
        self.started = []

    def place(self, name):
        return self.names.setdefault(name, len(self.names))

    def start(self, name, pairs, target):
        at = self.place(name)
        for source, destination in pairs:
            copy = pltpu.make_async_remote_copy(
                src_ref=source,
                dst_ref=destination,
                send_sem=self.send_sems.at[at],
                recv_sem=self.recv_sems.at[at],
                device_id=target,
                device_id_type=MESH,
            )
            copy.start()
        self.started.append(at)

    def wait(self, name, whole):
        at = self.place(name)
        pltpu.make_async_copy(whole, whole, self.recv_sems.at[at]).wait()

    def drain(self, name, whole):
        at = self.place(name)
        pltpu.make_async_copy(whole, whole, self.send_sems.at[at]).wait()


def gather_kernel(
    plan,
    hidden_ref,
    upstream_ref,
    weight_ref,
    matrix_ref,
    gain_ref,
    query_gain_ref,
    key_gain_ref,
    cosine_ref,
    sine_ref,
    normed_all,
    upstream_all,
    weight_full,
    matrix_full,
    weight_other,
    raw_ref,
    context_ref,
    context_grad_ref,
    normed_held,
    upstream_held,
    weight_near,
    matrix_near,
    tokens_near,
    context_sum,
    send_sems,
    recv_sems,
    local_sems,
    near_sems,
):
    head_bits, outer_bits, ranks, heads, cluster = plan
    gains_ref = (query_gain_ref, key_gain_ref)
    device = lax.axis_index("dp")
    plane = lax.axis_index("tensor")
    length, model = hidden_ref.shape
    rows = weight_ref.shape[0]
    parts = 2 ** len(head_bits)
    bits = head_bits + outer_bits
    slot_bits = head_bits[::-1]
    group = masks_of(head_bits)
    copies = Copies(send_sems, recv_sems)
    shared = ranks == 2 and any(bit > 1 for bit in head_bits)

    targets = [{"dp": flipped(device, mask, bits)} for mask in group[1:] + outer_bits]
    if shared:
        targets.append({"tensor": 1 - plane})
    barrier = pltpu.get_barrier_semaphore()
    for target in targets:
        pl.semaphore_signal(barrier, inc=1, device_id=target, device_id_type=MESH)
    pl.semaphore_wait(barrier, len(targets))

    def segments(full, ref):
        if full is weight_full:
            keys = KEY_VALUE_HEADS // ranks * HEAD_SIZE
            queries = QUERY_HEADS // ranks * HEAD_SIZE
            return [
                (0, queries // parts, 0),
                (queries, keys // parts, queries // parts),
                (queries + keys, keys // parts, (queries + keys) // parts),
            ]
        return [(0, ref.shape[1] // parts, 0)]

    def own_pairs(full, ref, mask):
        part = index_of(flipped(device, mask, bits), head_bits)
        first = pl.multiple_of(index_of(device, slot_bits) * rows, rows)
        pairs = []
        for start, width, place in segments(full, ref):
            source = ref.at[:, pl.ds(pl.multiple_of(start + part * width, HEAD_SIZE), width)]
            pairs.append((source, full.at[pl.ds(first, rows), pl.ds(place, width)]))
        return pairs

    def item(full, relative, mask):
        slot = index_of(flipped(device, mask, bits), slot_bits)
        first = pl.multiple_of((relative * parts + slot) * rows, rows)
        return full.at[pl.ds(first, rows), :]

    def base_start(name, full, ref):
        for mask in group[:0:-1]:
            copies.start((name, 0, mask), own_pairs(full, ref, mask), {"dp": flipped(device, mask, bits)})

    def outer_start(name, full, relative, mask, first_stage):
        for stage in range(first_stage, len(outer_bits)):
            bit = outer_bits[stage]
            landed = relative + 2**stage
            copies.start(
                (name, landed, mask),
                [(item(full, relative, mask), item(full, landed, mask))],
                {"dp": flipped(device, bit, bits)},
            )
        if full is weight_full and parts > 1:
            copies.start(
                ("x", relative, mask),
                [(item(full, relative, mask), item(weight_other, relative, mask))],
                {"dp": flipped(device, 1, bits)},
            )

    def arrive(name, full, relative, mask):
        copies.wait((name, relative, mask), item(full, relative, mask))
        stage = relative.bit_length()
        outer_start(name, full, relative, mask, stage)

    def place_own(full, ref, sem):
        pairs = own_pairs(full, ref, 0)
        for source, destination in pairs:
            pltpu.make_async_copy(source, destination, sem).start()

    def own_done(full, sem):
        whole = item(full, 0, 0)
        pltpu.make_async_copy(whole, whole, sem).wait()

    def sequence(full, index):
        return full.at[pl.ds(index * length, length), :]

    pieces = 2 if shared else 1
    height = length // (2 * pieces) if shared else length

    def piece_of(full, index, which, at):
        first = pl.multiple_of(index * length + (which * pieces + at) * height, height)
        return full.at[pl.ds(first, height), :]

    token_bits = head_bits[::-1]
    far = [bit for bit in token_bits if bit != 1]
    near = 2 ** len(far) if 1 in token_bits else 0

    here, there = (plane, 1 - plane) if shared else (0, 0)
    sibling = {"dp": flipped(device, 1, bits)}

    def tokens_start(name, full):
        if far:
            target = {"dp": flipped(device, far[0], bits)}
            for at in range(pieces):
                pair = (piece_of(full, 0, here, at), piece_of(full, 1, here, at))
                copies.start((name, "far", at), [pair], target)
        if near:
            copies.start((name, "near"), [(sequence(full, 0), sequence(full, near))], sibling)

    def tokens_far(name, full, at):
        if not far:
            return
        piece = piece_of(full, 1, here, at)
        copies.wait((name, "far", at), piece)
        if shared:
            copies.start((name, "side", at), [(piece, piece)], {"tensor": 1 - plane})
        if near:
            copies.start((name, "cross", at), [(piece, piece_of(full, near + 1, here, at))], sibling)

    def tokens_side(name, full, at):
        if not (far and shared):
            return
        piece = piece_of(full, 1, there, at)
        copies.wait((name, "side", at), piece)
        if near:
            copies.start((name, "over", at), [(piece, piece_of(full, near + 1, there, at))], sibling)

    def tokens_end(name, full):
        if near:
            copies.wait((name, "near"), sequence(full, near))
            for at in range(pieces if far else 0):
                copies.wait((name, "cross", at), piece_of(full, near + 1, here, at))
                if shared:
                    copies.wait((name, "over", at), piece_of(full, near + 1, there, at))

    relatives = list(range(1, 2 ** len(outer_bits)))
    last = 2 ** (len(outer_bits) - 1)
    early = [relative for relative in relatives if relative < last]
    late = [relative for relative in relatives if relative >= last]

    base_start("w", weight_full, weight_ref)
    place_own(weight_full, weight_ref, local_sems.at[0])
    own_done(weight_full, local_sems.at[0])

    inverse = lax.rsqrt(
        jnp.mean(jnp.square(hidden_ref[...].astype(F32)), axis=-1, keepdims=True) + EPSILON
    )
    for relative in range(2 ** len(outer_bits)):
        for slot in range(parts):
            owner = 0 * device
            for at, bit in enumerate(slot_bits):
                owner = owner + bit * ((slot >> at) & 1)
            for at, bit in enumerate(outer_bits):
                flag = bit_of(device, bit)
                owner = owner + bit * (flag + ((relative >> at) & 1) * (1 - 2 * flag))
            source = pl.ds(pl.multiple_of(owner * rows, rows), rows)
            target = pl.ds((relative * parts + slot) * rows, rows)
            piece = hidden_ref[:, source].astype(F32) * inverse * gain_ref[:, source]
            normed_held[:, target] = piece.astype(BF16)
            upstream_held[:, target] = upstream_ref[:, source]
    held_normed = pltpu.make_async_copy(normed_held, sequence(normed_all, 0), local_sems.at[1])
    held_normed.start()
    held_upstream = pltpu.make_async_copy(upstream_held, sequence(upstream_all, 0), local_sems.at[2])
    held_upstream.start()
    held_normed.wait()
    tokens_start("n", normed_all)
    outer_start("w", weight_full, 0, 0, 0)
    for mask in group[1:]:
        arrive("w", weight_full, 0, mask)
    held_upstream.wait()
    tokens_start("u", upstream_all)
    base_start("m", matrix_full, matrix_ref)
    place_own(matrix_full, matrix_ref, local_sems.at[3])
    own_done(matrix_full, local_sems.at[3])
    for at in range(pieces):
        tokens_far("n", normed_all, at)
    waiting = [(relative, mask) for relative in early for mask in group]
    for relative, mask in waiting[: len(waiting) // 2]:
        arrive("w", weight_full, relative, mask)
    for at in range(pieces):
        tokens_side("n", normed_all, at)
    for relative, mask in waiting[len(waiting) // 2 :]:
        arrive("w", weight_full, relative, mask)
    outer_start("m", matrix_full, 0, 0, 0)
    for relative in late:
        for mask in group:
            arrive("w", weight_full, relative, mask)
    load_weight = pltpu.make_async_copy(weight_full, weight_near, local_sems.at[4])
    load_weight.start()
    tokens_end("n", normed_all)

    def token_copy(full, index, columns):
        slot = lax.rem(index, 2)
        rows_of = pl.ds(pl.multiple_of(index * length, length), length)
        return pltpu.make_async_copy(
            full.at[rows_of, columns], tokens_near.at[slot, :, columns], near_sems.at[slot]
        )

    everything = pl.ds(0, model)
    token_copy(normed_all, 0, everything).start()
    load_weight.wait()

    def forward_step(index, carry):
        @pl.when(index + 1 < parts)
        def _():
            token_copy(normed_all, index + 1, everything).start()

        token_copy(normed_all, index, everything).wait()
        span = pl.ds(pl.multiple_of(index * length, length), length)
        raw_ref[span, :] = matmul(tokens_near[lax.rem(index, 2)], weight_near[...], (1, 0))
        forward_kernel(
            heads,
            cluster,
            min(length, ROW_BLOCK),
            raw_ref.at[span],
            gains_ref,
            cosine_ref,
            sine_ref,
            context_ref.at[span],
        )

        for at in range(pieces):

            @pl.when(index == max(parts - 3 + at, 0))
            def _(at=at):
                tokens_far("u", upstream_all, at)

        return carry

    lax.fori_loop(0, parts, forward_step, 0)
    for mask in group[1:]:
        arrive("m", matrix_full, 0, mask)
    for at in range(pieces):
        tokens_side("u", upstream_all, at)
    for relative in early:
        for mask in group:
            arrive("m", matrix_full, relative, mask)

    def context_half(which):
        columns = pl.ds(which * (model // 2), model // 2)
        load = pltpu.make_async_copy(
            matrix_full.at[columns, :], matrix_near.at[columns, :], local_sems.at[5 + which]
        )
        load.start()
        token_copy(upstream_all, 0, columns).start()
        load.wait()

        def step(index, carry):
            @pl.when(index + 1 < parts)
            def _():
                token_copy(upstream_all, index + 1, columns).start()

            token_copy(upstream_all, index, columns).wait()
            span = pl.ds(pl.multiple_of(index * length, length), length)
            part = matmul(tokens_near[lax.rem(index, 2), :, columns], matrix_near[columns, :], (1, 0))
            if which == 0:
                context_sum[span, :] = part
            else:
                context_grad_ref[span, :] = (context_sum[span, :] + part).astype(BF16)
            return carry

        lax.fori_loop(0, parts, step, 0)

    tokens_end("u", upstream_all)
    context_half(0)
    for relative in late:
        for mask in group:
            arrive("m", matrix_full, relative, mask)
    context_half(1)
    if parts > 1:
        for relative in range(2 ** len(outer_bits)):
            for mask in group:
                copies.wait(("x", relative, mask), item(weight_other, relative, mask))
                copies.drain(("x", relative, mask), item(weight_other, relative, mask))

    for name, full in (("w", weight_full), ("m", matrix_full)):
        for relative in range(2 ** len(outer_bits)):
            for mask in group:
                if relative or mask:
                    copies.drain((name, relative, mask), item(full, 0, 0))
    for name, full in (("n", normed_all), ("u", upstream_all)):
        for at in range(pieces if far else 0):
            piece = piece_of(full, 0, 0, 0)
            copies.drain((name, "far", at), piece)
            if shared:
                copies.drain((name, "side", at), piece)
            if near:
                copies.drain((name, "cross", at), piece)
                if shared:
                    copies.drain((name, "over", at), piece)
        if near:
            copies.drain((name, "near"), sequence(full, 0))


def gather_all(plan, hidden_in, upstream, weight, matrix, norm_gain, gains, cosine, sine):
    head_bits, outer_bits = plan[:2]
    length, model = hidden_in.shape
    parts = 2 ** len(head_bits)
    wide, narrow = weight.shape[1] // parts, matrix.shape[1] // parts
    count = 3 * (2 ** (len(outer_bits) + len(head_bits))) + 24
    anywhere = pl.BlockSpec(memory_space=pl.ANY)
    inside = pl.BlockSpec(memory_space=pltpu.VMEM)
    return pl.pallas_call(
        partial(gather_kernel, plan),
        in_specs=[inside] * 9,
        out_specs=[anywhere] * 5 + [inside] * 3,
        out_shape=[
            jax.ShapeDtypeStruct((parts * length, model), BF16),
            jax.ShapeDtypeStruct((parts * length, model), BF16),
            jax.ShapeDtypeStruct((model, weight.shape[1] // parts), BF16),
            jax.ShapeDtypeStruct((model, matrix.shape[1] // parts), BF16),
            jax.ShapeDtypeStruct((model if parts > 1 else 16, wide), BF16),
            jax.ShapeDtypeStruct((parts * length, wide), F32),
            jax.ShapeDtypeStruct((parts * length, narrow), BF16),
            jax.ShapeDtypeStruct((parts * length, narrow), BF16),
        ],
        scratch_shapes=[
            pltpu.VMEM((length, model), BF16),
            pltpu.VMEM((length, model), BF16),
            pltpu.VMEM((model, wide), BF16),
            pltpu.VMEM((model, narrow), BF16),
            pltpu.VMEM((2, length, model), BF16),
            pltpu.VMEM((parts * length, narrow), F32),
            pltpu.SemaphoreType.DMA((count,)),
            pltpu.SemaphoreType.DMA((count,)),
            pltpu.SemaphoreType.DMA((8,)),
            pltpu.SemaphoreType.DMA((2,)),
        ],
        compiler_params=pltpu.CompilerParams(
            collective_id=0, has_side_effects=True, vmem_limit_bytes=60 * 1024 * 1024
        ),
        cost_estimate=pl.CostEstimate(
            flops=10**11, bytes_accessed=64 * length * model, transcendentals=length
        ),
        name="gather_all",
    )(hidden_in, upstream, weight, matrix, norm_gain.reshape(1, model), *gains, cosine, sine)


def scatter_kernel(
    plan,
    upstream_all,
    normed_all,
    weight_full,
    weight_other,
    context_ref,
    context_grad_ref,
    raw_ref,
    query_gain_ref,
    key_gain_ref,
    cosine_ref,
    sine_ref,
    hidden_in,
    upstream_in,
    gain_ref,
    output_ref,
    input_ref,
    total_ref,
    sums_ref,
    gain_grad_ref,
    grad_ref,
    grad_other,
    left_held,
    weight_held,
    output_stage,
    output_landed,
    input_stage,
    input_landed,
    output_last,
    output_final,
    input_last,
    input_final,
    share_block,
    share_sent,
    share_got,
    share_own,
    share_far,
    send_sems,
    recv_sems,
    left_sems,
    weight_sems,
    leave_sems,
    gain_sent,
    gain_got,
):
    head_bits, outer_bits, ranks, heads, group = plan
    gains_ref = (query_gain_ref, key_gain_ref)
    device = lax.axis_index("dp")
    plane = lax.axis_index("tensor")
    parts = 2 ** len(head_bits)
    relatives = 2 ** len(outer_bits)
    length = cosine_ref.shape[0]
    model = weight_full.shape[0]
    rows = model // (parts * relatives)
    bits = head_bits + outer_bits
    slot_bits = head_bits[::-1]
    masks = masks_of(head_bits)
    scale = 1.0 / math.sqrt(lax.axis_size("dp") * length)
    copies = Copies(send_sems, recv_sems)

    outer_masks = masks_of(outer_bits)[1:] if parts > 1 else outer_bits
    targets = [{"dp": flipped(device, mask, bits)} for mask in masks[1:] + outer_masks]
    if parts > 1:
        targets.append({"tensor": 1 - plane})
    barrier = pltpu.get_barrier_semaphore()
    for target in targets:
        pl.semaphore_signal(barrier, inc=1, device_id=target, device_id_type=MESH)
    pl.semaphore_wait(barrier, len(targets))

    kinds = {
        "o": (upstream_all, context_ref, output_stage, output_landed, output_last, output_final, output_ref),
        "g": (normed_all, grad_ref, input_stage, input_landed, input_last, input_final, input_ref),
    }
    blocks = {"o": 0, "g": (relatives - 1) * parts + parts - 1}
    block_count = (relatives - 1) * parts + parts - 1

    def partner(mask_index):
        target, slot = device, 0 * device
        for at, bit in enumerate(head_bits):
            change = (mask_index // 2**at) % 2
            flag = bit_of(device, bit)
            target = target + bit * change * (1 - 2 * flag)
            slot = slot + 2 ** slot_bits.index(bit) * (flag + change - 2 * flag * change)
        return target, slot

    def left_copy(kind, relative, index):
        _, slot = partner(index)
        first = pl.multiple_of((relative * parts + slot) * rows, rows)
        return pltpu.make_async_copy(
            kinds[kind][0].at[:, pl.ds(first, rows)],
            left_held.at[lax.rem(index, 2)],
            left_sems.at[lax.rem(index, 2)],
        )

    def remote(kind, at, source, destination, target):
        return pltpu.make_async_remote_copy(
            src_ref=source,
            dst_ref=destination,
            send_sem=send_sems.at[blocks[kind] + at],
            recv_sem=recv_sems.at[blocks[kind] + at],
            device_id=target,
            device_id_type=MESH,
        )

    turns = [("o", relative) for relative in range(relatives - 1, 0, -1)]
    turns += [("g", relative) for relative in range(relatives - 1, 1, -1)]
    turns += [("o", 0), ("g", 1), ("g", 0)]
    left_copy(*turns[0], 0).start()

    def handle(kind, relative, index):
        _, right, stage, landed, last, final, result = kinds[kind]

        @pl.when(index + 1 < parts)
        def _():
            left_copy(kind, relative, index + 1).start()

        left_copy(kind, relative, index).wait()
        total = matmul(left_held[lax.rem(index, 2)], right[...], (0, 0))
        top = relative.bit_length()
        for later in range(top, len(outer_bits)):
            source = relative + 2**later
            at = (source - 1) * parts + index
            piece = landed.at[at]
            pltpu.make_async_copy(piece, piece, recv_sems.at[blocks[kind] + at]).wait()
            total = total + piece[...].astype(F32)
        if relative:
            at = (relative - 1) * parts + index
            stage[at] = total.astype(BF16)
            target = {"dp": flipped(device, outer_bits[top - 1], bits)}
            remote(kind, at, stage.at[at], landed.at[at], target).start()
        else:
            last[index] = total.astype(BF16)

            @pl.when(index > 0)
            def _():
                target, _ = partner(index)
                at = (relatives - 1) * parts + index - 1
                remote(kind, at, last.at[index], final.at[index - 1], {"dp": target}).start()

        following = turns.index((kind, relative)) + 1
        if following < len(turns):

            @pl.when(index + 1 == parts)
            def _():
                left_copy(*turns[following], 0).start()

    def process(kind, relative):
        def body(index, carry):
            handle(kind, relative, index)
            return carry

        lax.fori_loop(0, parts, body, 0)

    for relative in range(relatives - 1, 1, -1):
        process("o", relative)


    def sequence_step(index, carry):
        span = pl.ds(pl.multiple_of(index * length, length), length)
        backward_kernel(
            heads,
            group,
            min(length, ROW_BLOCK),
            raw_ref.at[span],
            context_grad_ref.at[span],
            gains_ref,
            cosine_ref,
            sine_ref,
            grad_ref.at[span],
            sums_ref,
            index,
        )
        handle("o", 1, index)
        return carry

    lax.fori_loop(0, parts, sequence_step, 0)

    if parts > 1:
        near = (parts // 2) * length
        copies.names = {("skip", at): at for at in range(2 * block_count)}
        copies.start(
            "grad",
            [(grad_ref.at[pl.ds(near, near)], grad_other)],
            {"dp": flipped(device, 1, bits)},
        )

    width = weight_held.shape[2]
    weight_blocks = model // width

    def weight_copies(index):
        slot = lax.rem(index, 2)
        span = pl.ds(pl.multiple_of(index * width, width), width)
        pairs = [(weight_full, 0)] + ([(weight_other, 1)] if parts > 1 else [])
        return [
            pltpu.make_async_copy(full.at[span], weight_held.at[slot, at], weight_sems.at[slot, at])
            for full, at in pairs
        ]

    half = length // 2
    mine = pl.ds(pl.multiple_of(plane % 2 * half, half), half)
    theirs = pl.ds(pl.multiple_of((1 - plane % 2) * half, half), half)
    taken = (parts // 2) * length if parts > 1 else length

    for copy in weight_copies(0):
        copy.start()
    if parts > 1:
        copies.wait("grad", grad_other)

    side = {"tensor": 1 - plane}
    halves = [pl.ds(at * (model // 2), model // 2) for at in range(2)]

    def side_start(at):
        copies.start(
            ("side", at),
            [(share_sent.at[0, :, halves[at]], share_got.at[0, :, halves[at]])],
            side,
        )

    def weight_step(index, carry):
        @pl.when(index + 1 < weight_blocks)
        def _():
            for copy in weight_copies(index + 1):
                copy.start()

        for copy in weight_copies(index):
            copy.wait()
        slot = lax.rem(index, 2)
        span = pl.ds(pl.multiple_of(index * width, width), width)
        share = matmul(grad_ref[0:taken], weight_held[slot, 0], (1, 1))
        if parts > 1:
            share = share + matmul(grad_other[...], weight_held[slot, 1], (1, 1))
            share_block[...] = share
            far_mine = pl.ds(pl.multiple_of(length + plane % 2 * half, half), half)
            far_theirs = pl.ds(pl.multiple_of(length + (1 - plane % 2) * half, half), half)
            share_far[:, span] = share_block[far_mine, :].astype(BF16)
            share_sent[0, :, span] = share_block[far_theirs, :].astype(BF16)
            share_own[:, span] = share_block[mine, :].astype(BF16)
            share_sent[1, :, span] = share_block[theirs, :].astype(BF16)

            @pl.when(index == weight_blocks // 2 - 1)
            def _():
                side_start(0)

            @pl.when(index == weight_blocks - 1)
            def _():
                side_start(1)

        else:
            total_ref[:, span] = share.astype(BF16)
        return carry

    lax.fori_loop(0, weight_blocks, weight_step, 0)
    across = {"dp": flipped(device, 4, bits)}

    def across_start(at):
        where = halves[at]
        copies.wait(("side", at), share_got.at[0, :, where])
        share_far[:, where] = (
            share_far[:, where].astype(F32) + share_got[0, :, where].astype(F32)
        ).astype(BF16)
        copies.start(
            ("across", at), [(share_far.at[:, where], share_got.at[2, :, where])], across
        )

    def back_start(at):
        where = halves[at]
        copies.wait(("across", at), share_got.at[2, :, where])
        share_own[:, where] = (
            share_own[:, where].astype(F32)
            + share_got[1, :, where].astype(F32)
            + share_got[2, :, where].astype(F32)
        ).astype(BF16)
        total_ref[mine, where] = share_own[:, where]
        copies.start(
            ("back", at), [(share_own.at[:, where], total_ref.at[mine, where])], side
        )

    if parts > 1:
        copies.start("rest", [(share_sent.at[1], share_got.at[1])], side)
    for relative in range(relatives - 1, 1, -1):
        process("g", relative)
    if parts > 1:
        across_start(0)
    process("o", 0)
    if parts > 1:
        across_start(1)
    if relatives > 1:
        process("g", 1)
    if parts > 1:
        copies.wait("rest", share_got.at[1])
        back_start(0)
        back_start(1)
        copies.drain("rest", share_own)
        for name in ("side", "across"):
            for at in range(2):
                copies.drain((name, at), share_far.at[:, halves[at]])
        gain_grad_ref[...] = jnp.zeros_like(gain_grad_ref)
        loads = [
            pltpu.make_async_copy(full.at[where], buffer, leave_sems.at[at])
            for at, (full, where, buffer) in enumerate(
                [
                    (hidden_in, mine, share_sent.at[0]),
                    (upstream_in, mine, share_sent.at[1]),
                    (hidden_in, theirs, share_got.at[0]),
                    (upstream_in, theirs, share_got.at[1]),
                ]
            )
        ]
        for load in loads:
            load.start()
        for load in loads:
            load.wait()

    owners = []
    for relative in range(relatives):
        for slot in range(parts):
            owner = 0 * device
            for at, bit in enumerate(slot_bits):
                owner = owner + bit * ((slot >> at) & 1)
            for at, bit in enumerate(outer_bits):
                flag = bit_of(device, bit)
                owner = owner + bit * (flag + ((relative >> at) & 1) * (1 - 2 * flag))
            owners.append(owner)

    def leave_half(first_row, buffers):
        step_rows = 32

        def step(index, carry):
            there = pl.ds(pl.multiple_of(first_row + index * step_rows, step_rows), step_rows)
            span = pl.ds(pl.multiple_of(index * step_rows, step_rows), step_rows)
            for at, owner in enumerate(owners):
                share_far[span, pl.ds(pl.multiple_of(owner * rows, rows), rows)] = total_ref[
                    there, at * rows : (at + 1) * rows
                ]
            states = buffers[0][span, :].astype(F32)
            inverse = lax.rsqrt(jnp.mean(states * states, axis=-1, keepdims=True) + EPSILON)
            unit = states * inverse
            grad = share_far[span, :].astype(F32)
            gain_grad_ref[...] += jnp.sum(grad * unit, axis=0, keepdims=True)
            scaled = grad * gain_ref[...]
            mean = jnp.mean(scaled * unit, axis=-1, keepdims=True)
            result = buffers[1][span, :].astype(F32) + inverse * (scaled - unit * mean)
            total_ref[there, :] = result.astype(BF16)
            return carry

        lax.fori_loop(0, half // step_rows, step, 0)

    if parts > 1:
        leave_half(plane % 2 * half, (share_sent.at[0], share_sent.at[1]))
    process("g", 0)

    def finish(kind, indices):
        _, _, stage, _, last, final, result = kinds[kind]
        if kind == "o":
            spans = [(0, heads * group * HEAD_SIZE, 0)]
        else:
            query, key = heads * group * HEAD_SIZE, heads * HEAD_SIZE
            spans = [
                (0, query, 0),
                (query, key, parts * query),
                (query + key, key, parts * (query + key)),
            ]
        for index in indices:
            if index:
                at = (relatives - 1) * parts + index - 1
                piece = final.at[index - 1]
                pltpu.make_async_copy(piece, piece, recv_sems.at[blocks[kind] + at]).wait()
            values = (last[0] if index == 0 else final[index - 1]).astype(F32) * scale
            part = index_of(flipped(device, masks[index], bits), head_bits)
            for start, columns, place in spans:
                result[:, pl.ds(pl.multiple_of(place + part * columns, HEAD_SIZE), columns)] = values[
                    :, start : start + columns
                ]

    finish("o", range(parts))
    if parts > 1:
        for at in range(2):
            copies.wait(("back", at), total_ref.at[theirs, halves[at]])
        leave_half((1 - plane % 2) * half, (share_got.at[0], share_got.at[1]))
        gain_sent[0, :, :model] = gain_grad_ref[...] * (1.0 / ranks)
        gain_sent[0, :, model : model + HEAD_SIZE] = sums_ref[0:1]
        gain_sent[0, :, model + HEAD_SIZE :] = sums_ref[1:2]
        stages = [
            [{"dp": flipped(device, mask, bits)} for mask in masks[1:]],
            [{"dp": flipped(device, mask, bits)} for mask in outer_masks],
            [side],
        ]

        def gains_start(stage):
            for at, target in enumerate(stages[stage]):
                copies.start(
                    ("gain", stage, at),
                    [(gain_sent.at[stage], gain_got.at[3 * stage + at])],
                    target,
                )

        def gains_end(stage):
            terms = [gain_sent[stage]]
            for at in range(len(stages[stage])):
                place = gain_got.at[3 * stage + at]
                copies.wait(("gain", stage, at), place)
                terms.append(place[...])
            while len(terms) > 1:
                terms = [terms[at] + terms[at + 1] for at in range(0, len(terms), 2)]
            return terms[0]

        gains_start(0)
        finish("g", range(0, 2))
        gain_sent[1] = gains_end(0)
        gains_start(1)
        finish("g", range(2, parts))
        gain_sent[2] = gains_end(1)
        gains_start(2)
        gain_total = gains_end(2) * scale
        gain_grad_ref[...] = gain_total[:, :model]
        sums_ref[0:1] = gain_total[:, model : model + HEAD_SIZE]
        sums_ref[1:2] = gain_total[:, model + HEAD_SIZE :]
        for stage in range(3):
            for at in range(len(stages[stage])):
                copies.drain(("gain", stage, at), gain_sent.at[0])
    else:
        gain_grad_ref[...] = jnp.zeros_like(gain_grad_ref)
        finish("g", range(parts))

    for kind in ("o", "g"):
        _, _, stage, _, last, _, _ = kinds[kind]
        for at in range(block_count):
            piece = stage.at[0]
            pltpu.make_async_copy(piece, piece, send_sems.at[blocks[kind] + at]).wait()
    if parts > 1:
        copies.drain("grad", grad_other)
        for at in range(2):
            copies.drain(("back", at), share_far.at[:, halves[at]])


def scatter_all(plan, upstream_all, normed_all, weight_full, weight_other, *rest):
    context, _, raw, _, _, cosine = rest[:6]
    head_bits, outer_bits, ranks, heads, group = plan
    parts = 2 ** len(head_bits)
    relatives = 2 ** len(outer_bits)
    length = cosine.shape[0]
    model = weight_full.shape[0]
    rows = model // (parts * relatives)
    tokens = raw.shape[0]
    narrow, wide = context.shape[1], raw.shape[1]
    block_count = (relatives - 1) * parts + parts - 1
    half, width = length // 2, min(256, model)
    near = max(parts // 2, 1) * length
    anywhere = pl.BlockSpec(memory_space=pl.ANY)
    inside = pl.BlockSpec(memory_space=pltpu.VMEM)
    staged = max((relatives - 1) * parts, 1)
    spare = max(parts - 1, 1)
    many = parts > 1
    return pl.pallas_call(
        partial(scatter_kernel, plan),
        in_specs=[anywhere] * 4 + [inside] * 7 + [anywhere] * 2 + [inside],
        out_specs=[inside] * 5,
        out_shape=[
            jax.ShapeDtypeStruct((rows, parts * narrow), F32),
            jax.ShapeDtypeStruct((rows, parts * wide), F32),
            jax.ShapeDtypeStruct((length, model), BF16),
            jax.ShapeDtypeStruct((2, HEAD_SIZE), F32),
            jax.ShapeDtypeStruct((1, model), F32),
        ],
        scratch_shapes=[
            pltpu.VMEM((tokens, wide), BF16),
            pltpu.VMEM((near, wide) if many else (16, 128), BF16),
            pltpu.VMEM((2, tokens, rows), BF16),
            pltpu.VMEM((2, 2, width, wide), BF16),
            pltpu.VMEM((staged, rows, narrow), BF16),
            pltpu.VMEM((staged, rows, narrow), BF16),
            pltpu.VMEM((staged, rows, wide), BF16),
            pltpu.VMEM((staged, rows, wide), BF16),
            pltpu.VMEM((parts, rows, narrow), BF16),
            pltpu.VMEM((spare, rows, narrow), BF16),
            pltpu.VMEM((parts, rows, wide), BF16),
            pltpu.VMEM((spare, rows, wide), BF16),
            pltpu.VMEM((near, width) if many else (16, 128), F32),
            pltpu.VMEM((2, half, model) if many else (2, 16, 128), BF16),
            pltpu.VMEM((3, half, model) if many else (3, 16, 128), BF16),
            pltpu.VMEM((half, model) if many else (16, 128), BF16),
            pltpu.VMEM((half, model) if many else (16, 128), BF16),
            pltpu.SemaphoreType.DMA((2 * block_count + 16,)),
            pltpu.SemaphoreType.DMA((2 * block_count + 16,)),
            pltpu.SemaphoreType.DMA((2,)),
            pltpu.SemaphoreType.DMA((2, 2)),
            pltpu.SemaphoreType.DMA((4,)),
            pltpu.VMEM((3, 1, model + 2 * HEAD_SIZE), F32),
            pltpu.VMEM((7, 1, model + 2 * HEAD_SIZE), F32),
        ],
        compiler_params=pltpu.CompilerParams(
            collective_id=1, has_side_effects=True, vmem_limit_bytes=63 * 1024 * 1024
        ),
        cost_estimate=pl.CostEstimate(
            flops=10**11, bytes_accessed=64 * length * model, transcendentals=length
        ),
        name="scatter_all",
    )(upstream_all, normed_all, weight_full, weight_other, *rest)


def local(hidden_in, upstream, merged_input_weight, output_matrix, norm_gain, query_gain, key_gain):
    shard_ranks = lax.axis_size("tensor")
    groups = lax.axis_size("dp")
    device = lax.axis_index("dp")
    key_heads = KEY_VALUE_HEADS // shard_ranks
    group_width = QUERY_HEADS // KEY_VALUE_HEADS
    length, model = hidden_in.shape
    grad_scale = 1.0 / math.sqrt(groups * length)
    bits = device_bits(groups)
    head_bits = [1, 4] if key_heads % 4 == 0 and groups >= 8 and shard_ranks == 2 else []
    outer_bits = [bit for bit in bits if bit > 2 and bit not in head_bits]
    outer_bits += [bit for bit in bits if bit <= 2 and bit not in head_bits]
    parts = 2 ** len(head_bits)
    part_keys = key_heads // parts
    cosine, sine = rope_tables(length, HEAD_SIZE)
    gains = (query_gain.reshape(1, HEAD_SIZE), key_gain.reshape(1, HEAD_SIZE))
    plan = (head_bits, outer_bits, shard_ranks, part_keys, group_width)
    gathered = gather_all(
        plan,
        hidden_in,
        upstream,
        merged_input_weight,
        output_matrix,
        norm_gain,
        gains,
        cosine,
        sine,
    )
    normed_all, upstream_all, weight_full, _, weight_other = gathered[:5]
    projected, context_low, context_gradient = gathered[5:]
    output_grad, input_grad, hidden_grad, head_sums, gain_part = scatter_all(
        plan,
        upstream_all,
        normed_all,
        weight_full,
        weight_other,
        context_low,
        context_gradient,
        projected,
        *gains,
        cosine,
        sine,
        hidden_in,
        upstream,
        norm_gain.reshape(1, model),
    )
    if parts == 1:
        shares = [hidden_grad]
        for shift in range(1, shard_ranks):
            pairs = [(i, (i + shift) % shard_ranks) for i in range(shard_ranks)]
            shares.append(lax.ppermute(hidden_grad, "tensor", pairs))
        places = jnp.stack(block_places(head_bits, outer_bits, device)).astype(jnp.int32)
        hidden_grad, gain_part = leave(places, hidden_in, upstream, norm_gain, shares)
        sums = jnp.concatenate([gain_part * (1.0 / shard_ranks), head_sums[0], head_sums[1]])
        sums = sum_all(sum_all(sums, "tensor"), "dp") * grad_scale
        gain_grad, query_grad, key_grad = jnp.split(sums, [model, model + HEAD_SIZE])
    else:
        gain_grad, query_grad, key_grad = gain_part[0], head_sums[0], head_sums[1]
    return (
        hidden_grad,
        input_grad,
        output_grad,
        gain_grad,
        query_grad,
        key_grad,
    )


def solution(mesh):
    in_specs = (P("dp", None), P("dp", None), P("dp", "tensor"), P("dp", "tensor"), P(), P(), P())
    out_specs = (P("dp", None), P("dp", "tensor"), P("dp", "tensor"), P(), P(), P())
    return jax.shard_map(local, mesh=mesh, in_specs=in_specs, out_specs=out_specs, check_vma=False)
```
